512 devices in a mesh: tbl: 32 (over z, core), grp: 16 (over y, x).
Axes of the slice: x: 4, y: 4, z: 16, core: 2. Of those that a mesh axis runs over, the one named last changes fastest.
Arguments:
- codes: bfloat16 [32, 4096, 256], P('tbl', 'grp'), may hold values from -4 to 4
- row_scales: float32 [32, 4096], P('tbl', 'grp'), may hold values from 0.25 to 16
- history_lengths: int32 [512, 32], P(None, 'tbl'), may hold values from 1 to 32, as said below
- history_ids: int32 [512, 32, 32], P(None, 'tbl'), may hold values from 0 to 4095, as said below
- query_items: int32 [512, 32], P(None, 'tbl'), may hold values from 0 to 4095, as said below
- slot_tables: int32 [32], replicated, may hold values from 0 to 31, each once
Outputs:
- pooled: bfloat16 [512, 32, 256], P(('tbl', 'grp'))
The draws below stay inside these ranges and needn't reach their ends.
Inputs may be any that keep to these rules, and one draw needn't show every extreme that they name: `history_lengths`: the largest length, 32, occurs in every draw. `history_ids`: entries at positions at or beyond the history's length are row ids too, and are to be ignored. query_items[b, s] equals history_ids[b, s, h] for some h below history_lengths[b, s].
All inputs are finite; a program needn't handle non-finite values.
Results may differ from the reference program's by a relative error of at most 0.004.
Values may be sent and summed in bfloat16 or wider, within the bound.
No kernel may reach another device: no remote copies, remote signals or barrier semaphores. Data moves between devices by JAX's collectives and lax.ppermute only.
A program may use at most 64 MiB of HBM per device.

```python
import math
import jax
import jax.numpy as jnp
from jax import lax

E = 256
ROWS_DEV = 256
HMAX = 32
NT = 32
TROWS = 4096
BATCH = 512


def history_draw(key):
    length_key, owner_key, row_key, where_key = jax.random.split(jax.random.fold_in(key, 7), 4)
    lengths = jax.random.randint(length_key, (BATCH, NT), 1, HMAX + 1)
    sample_pos = jnp.arange(BATCH, dtype=jnp.int32)[:, None]
    slot_pos = jnp.arange(NT, dtype=jnp.int32)[None, :]
    lengths = jnp.where((sample_pos + 3 * slot_pos) % 61 == 0, HMAX, lengths)
    groups = TROWS // ROWS_DEV
    picked = jax.random.randint(owner_key, (BATCH, NT, HMAX), 0, 2 * groups)
    owner = (jnp.minimum(picked, groups - 1) + slot_pos[:, :, None]) % groups
    ids = owner * ROWS_DEV + jax.random.randint(row_key, (BATCH, NT, HMAX), 0, ROWS_DEV)
    target_pos = jax.random.randint(where_key, (BATCH, NT), 0, 1 << 20) % lengths
    target = jnp.take_along_axis(ids, target_pos[:, :, None], axis=2)[:, :, 0]
    partner_pos = (target_pos + 1) % lengths
    positions = jnp.arange(HMAX, dtype=jnp.int32)[None, None, :]
    pairing = (positions == partner_pos[:, :, None]) & (lengths[:, :, None] > 1)
    ids = jnp.where(pairing, jnp.bitwise_xor(target, 1)[:, :, None], ids)
    return (lengths.astype(jnp.int32), ids.astype(jnp.int32), target.astype(jnp.int32))


def draw_history_lengths(key, part):
    return history_draw(key)[0]


def draw_history_ids(key, part):
    return history_draw(key)[1]


def draw_query_items(key, part):
    return history_draw(key)[2]


def draw_codes(key, part):
    base_key = jax.random.fold_in(jax.random.fold_in(key, 11), 0)
    base = jnp.clip(jax.random.normal(base_key, (NT, TROWS, E), jnp.float32), -4.0, 4.0)
    return base.astype(jnp.bfloat16)


def draw_row_scales(key, part):
    first_key = jax.random.fold_in(jax.random.fold_in(key, 13), 0)
    return jnp.exp(jax.random.uniform(first_key, (NT, TROWS), jnp.float32, math.log(0.25), math.log(2.0)))


def setup_inputs(seed: int = 0) -> dict:
    splits = jax.random.split(jax.random.key(seed), 7)
    return {
        "codes": draw_codes(jax.random.fold_in(splits[6], 71), 0),
        "row_scales": draw_row_scales(jax.random.fold_in(splits[6], 71), 0),
        "history_lengths": draw_history_lengths(jax.random.fold_in(splits[6], 71), 0),
        "history_ids": draw_history_ids(jax.random.fold_in(splits[6], 71), 0),
        "query_items": draw_query_items(jax.random.fold_in(splits[6], 71), 0),
        "slot_tables": jax.random.permutation(splits[5], NT).astype(jnp.int32),
    }


def reference(codes, row_scales, history_lengths, history_ids, query_items, slot_tables):
    positions = jnp.arange(HMAX, dtype=jnp.int32)

    def one_slot(inputs):
        table, factors, ids, lengths, items = inputs
        found = jnp.take(table, ids, axis=0).astype(jnp.float32)
        factor = jnp.take(factors, ids, axis=0)
        query = jnp.take(table, items, axis=0).astype(jnp.float32) * jnp.take(factors, items, axis=0)[:, None]
        raw = jnp.einsum("bhe,be->bh", found, query, precision=lax.Precision.HIGHEST)
        score = raw * factor / E
        keep = positions[None, :] < lengths[:, None]
        peak = jnp.max(jnp.where(keep, score, -1e30), axis=1)
        weight = jnp.where(keep, jnp.exp(score - peak[:, None]), 0.0)
        weighted = jnp.einsum("bh,bhe->be", weight * factor, found, precision=lax.Precision.HIGHEST)
        return weighted / jnp.sum(weight, axis=1)[:, None]

    pooled_slot = lax.map(one_slot, (codes, row_scales, jnp.transpose(history_ids, (1, 0, 2)),
                                     jnp.transpose(history_lengths), jnp.transpose(query_items)))
    arranged = jnp.transpose(pooled_slot, (1, 0, 2)).astype(jnp.bfloat16)
    inverse = jnp.argsort(slot_tables).astype(jnp.int32)
    return jnp.take(arranged, inverse, axis=1)
```

```python
import jax
import jax.numpy as jnp
from jax import lax
from jax.experimental import pallas as pl
from jax.experimental.pallas import tpu as pltpu
from jax.sharding import PartitionSpec as P

F32 = jnp.float32
BF16 = jnp.bfloat16
VMEM = pl.BlockSpec(memory_space=pltpu.VMEM)
SMEM = pl.BlockSpec(memory_space=pltpu.SMEM)
SCALE_ROWS = 8


def pack_kernel(codes_ref, scales_ref, out_ref, block_ref, sems):
    copies, _, width = out_ref.shape
    rows = codes_ref.shape[0]
    scale = scales_ref[...]
    high = scale.astype(BF16)
    rest = scale - high.astype(F32)
    middle = rest.astype(BF16)
    low = (rest - middle.astype(F32)).astype(BF16)
    place = lax.broadcasted_iota(jnp.int32, (SCALE_ROWS, width), 0)
    terms = jnp.where(
        place == 0,
        high.astype(F32),
        jnp.where(place == 1, middle.astype(F32), jnp.where(place == 2, low.astype(F32), 0.0)),
    ).astype(BF16)
    block_ref[:rows, :] = codes_ref[...]
    block_ref[rows:, :] = terms
    moves = [
        pltpu.make_async_copy(block_ref, out_ref.at[copy], sems.at[copy]) for copy in range(copies)
    ]
    for move in moves:
        move.start()
    for move in moves:
        move.wait()


def count_kernel(grp_ref, ids_ref, lengths_ref, items_ref, counts_ref, target_ref):
    history, batch = ids_ref.shape
    samples, table_rows = counts_ref.shape
    grp_count = batch // samples
    ids = ids_ref[...]
    items = items_ref[...]
    extra = jnp.concatenate(
        [
            lengths_ref[...],
            lax.shift_right_logical(items, 6),
            jnp.bitwise_and(items, 63),
            jnp.zeros((5, batch), jnp.int32),
        ],
        axis=0,
    )
    digits = jnp.concatenate(
        [lax.shift_right_logical(ids, 6), jnp.bitwise_and(ids, 63), extra], axis=0
    )
    digits = digits.astype(F32).astype(BF16)
    sample = lax.broadcasted_iota(jnp.int32, (samples, batch), 0)
    column = lax.broadcasted_iota(jnp.int32, (samples, batch), 1)
    chosen = jnp.where(column == sample * grp_count + grp_ref[0], 1.0, 0.0).astype(BF16)
    own = lax.dot_general(chosen, digits, (((1,), (1,)), ((), ())), preferred_element_type=F32)
    own_ids = own[:, :history] * 64.0 + own[:, history : 2 * history]
    own_lengths = own[:, 2 * history : 2 * history + 1]
    own_items = own[:, 2 * history + 1 : 2 * history + 2] * 64.0 + own[:, 2 * history + 2 : 2 * history + 3]
    position = lax.broadcasted_iota(jnp.int32, (samples, history), 1).astype(F32)
    own_ids = jnp.where(position < own_lengths, own_ids, -1.0)
    lane = lax.broadcasted_iota(jnp.int32, (8, 128), 1).astype(F32)
    for first in range(0, samples, 8):
        names = [
            jnp.broadcast_to(own_ids[first : first + 8, h : h + 1], (8, 128)) for h in range(history)
        ]
        item = jnp.broadcast_to(own_items[first : first + 8], (8, 128))

        def tile(k, carry):
            row = lane + (k * 128).astype(F32)
            total = jnp.zeros((8, 128), F32)
            for h in range(history):
                total = total + jnp.where(names[h] == row, 1.0, 0.0)
            at = pl.ds(pl.multiple_of(k * 128, 128), 128)
            counts_ref[first : first + 8, at] = total
            target_ref[first : first + 8, at] = jnp.where(item == row, 1.0, 0.0)
            return carry

        lax.fori_loop(0, table_rows // 128, tile, 0, unroll=2)


def pool_kernel(table_ref, counts_ref, target_ref, out_ref, score_ref):
    blocks, height, width = table_ref.shape
    rows = height - SCALE_ROWS
    samples = counts_ref.shape[0]

    def scales(block):
        terms = table_ref[block, rows:, :].astype(F32)
        return terms[0:1] + (terms[1:2] + terms[2:3])

    query = jnp.zeros((samples, width), F32)
    factor = jnp.zeros((samples, rows), F32)
    for block in range(blocks):
        target = target_ref[:, block * rows : (block + 1) * rows]
        query = query + jnp.dot(
            target.astype(BF16), table_ref[block, :rows, :], preferred_element_type=F32
        )
        factor = factor + target * scales(block)
    query = query.astype(BF16)
    factor = jnp.sum(factor, axis=1, keepdims=True) * (1.0 / width)
    top = jnp.full((samples, rows), -1e30, F32)
    for block in range(blocks):
        raw = lax.dot_general(
            query, table_ref[block, :rows, :], (((1,), (1,)), ((), ())), preferred_element_type=F32
        )
        score = raw * scales(block) * factor
        at = slice(block * rows, (block + 1) * rows)
        score = jnp.where(counts_ref[:, at] > 0.0, score, -1e30)
        score_ref[:, at] = score
        top = jnp.maximum(top, score)
    peak = jnp.max(top, axis=1, keepdims=True)
    mass = jnp.zeros((samples, rows), F32)
    pooled = jnp.zeros((2 * samples, width), F32)
    for block in range(blocks):
        at = slice(block * rows, (block + 1) * rows)
        weight = counts_ref[:, at] * jnp.exp(score_ref[:, at] - peak)
        mass = mass + weight
        scaled = weight * scales(block)
        high = scaled.astype(BF16)
        low = (scaled - high.astype(F32)).astype(BF16)
        pooled = pooled + jnp.dot(
            jnp.concatenate([high, low], axis=0),
            table_ref[block, :rows, :],
            preferred_element_type=F32,
        )
    mass = jnp.sum(mass, axis=1, keepdims=True)
    out_ref[...] = ((pooled[:samples] + pooled[samples:]) / mass).astype(out_ref.dtype)


def order_kernel(tables_ref, pooled_ref, out_ref):
    slots = pooled_ref.shape[0]
    table = lax.broadcasted_iota(jnp.int32, (slots, slots), 0)
    place = jnp.where(table == tables_ref[...], 1.0, 0.0).astype(BF16)
    out_ref[0] = jnp.dot(place, pooled_ref[...], preferred_element_type=F32).astype(BF16)


def per_device(codes, row_scales, history_lengths, history_ids, query_items, slot_tables):
    _, rows, width = codes.shape
    batch, _, history = history_ids.shape
    tbl_count = lax.axis_size("tbl")
    grp_count = lax.axis_size("grp")
    samples = batch // grp_count
    table_rows = rows * grp_count
    packed = pl.pallas_call(
        pack_kernel,
        out_shape=jax.ShapeDtypeStruct((grp_count, rows + SCALE_ROWS, width), BF16),
        in_specs=[VMEM, VMEM],
        out_specs=pl.BlockSpec(memory_space=pltpu.HBM),
        scratch_shapes=[
            pltpu.VMEM((rows + SCALE_ROWS, width), BF16),
            pltpu.SemaphoreType.DMA((grp_count,)),
        ],
        compiler_params=pltpu.CompilerParams(vmem_limit_bytes=16 << 20),
        name="pack",
    )(codes[0], row_scales)
    table = lax.all_to_all(packed, "grp", split_axis=0, concat_axis=0, tiled=True)
    grp = lax.axis_index("grp").astype(jnp.int32).reshape(1)
    counts, target = pl.pallas_call(
        count_kernel,
        out_shape=[
            jax.ShapeDtypeStruct((samples, table_rows), F32),
            jax.ShapeDtypeStruct((samples, table_rows), F32),
        ],
        in_specs=[SMEM, VMEM, VMEM, VMEM],
        out_specs=[VMEM, VMEM],
        cost_estimate=pl.CostEstimate(flops=100_000_000, bytes_accessed=1_000_000, transcendentals=0),
        compiler_params=pltpu.CompilerParams(vmem_limit_bytes=16 << 20),
        name="count",
    )(grp, history_ids[:, 0, :].T, history_lengths.T, query_items.T)
    pooled = pl.pallas_call(
        pool_kernel,
        out_shape=jax.ShapeDtypeStruct((samples, width), BF16),
        in_specs=[VMEM, VMEM, VMEM],
        out_specs=VMEM,
        scratch_shapes=[pltpu.VMEM((samples, table_rows), F32)],
        compiler_params=pltpu.CompilerParams(vmem_limit_bytes=16 << 20),
        name="pool",
    )(table, counts, target)
    arrived = lax.all_to_all(pooled, "tbl", split_axis=0, concat_axis=0, tiled=True)
    return pl.pallas_call(
        order_kernel,
        out_shape=jax.ShapeDtypeStruct((1, tbl_count, width), BF16),
        in_specs=[VMEM, VMEM],
        out_specs=VMEM,
        compiler_params=pltpu.CompilerParams(vmem_limit_bytes=16 << 20),
        name="order",
    )(slot_tables.reshape(1, tbl_count), arrived)


def solution(mesh):
    placed = (
        P("tbl", "grp", None),
        P("tbl", "grp"),
        P(None, "tbl"),
        P(None, "tbl", None),
        P(None, "tbl"),
        P(),
    )
    return jax.shard_map(
        per_device,
        mesh=mesh,
        in_specs=placed,
        out_specs=P(("tbl", "grp"), None, None),
        check_vma=False,
    )
```

```python
import functools

import jax
import jax.numpy as jnp
from jax import lax
from jax.experimental import pallas as pl
from jax.experimental.pallas import tpu as pltpu
from jax.sharding import PartitionSpec as P

F32 = jnp.float32
BF16 = jnp.bfloat16
VMEM = pl.BlockSpec(memory_space=pltpu.VMEM)
SMEM = pl.BlockSpec(memory_space=pltpu.SMEM)
HBM = pl.BlockSpec(memory_space=pltpu.HBM)
SMALL = pltpu.CompilerParams(vmem_limit_bytes=16 << 20)
SCALE_ROWS = 8
LANES = 128


def rotated(count, first):
    return [(place + first) % count for place in range(count)]


def pack_kernel(codes_ref, scales_ref, out_ref, block_ref, scale_ref, sems):
    copies = out_ref.shape[0]
    rows, width = codes_ref.shape
    fetch = [
        pltpu.make_async_copy(codes_ref, block_ref.at[pl.ds(0, rows)], sems.at[copies]),
        pltpu.make_async_copy(scales_ref, scale_ref, sems.at[copies + 1]),
    ]
    for move in fetch:
        move.start()
    fetch[1].wait()
    scale = scale_ref[...]
    high = scale.astype(BF16)
    rest = scale - high.astype(F32)
    middle = rest.astype(BF16)
    low = (rest - middle.astype(F32)).astype(BF16)
    place = lax.broadcasted_iota(jnp.int32, (SCALE_ROWS, width), 0)
    terms = jnp.where(
        place == 0,
        high.astype(F32),
        jnp.where(place == 1, middle.astype(F32), jnp.where(place == 2, low.astype(F32), 0.0)),
    ).astype(BF16)
    block_ref[rows:, :] = terms
    fetch[0].wait()
    moves = [
        pltpu.make_async_copy(block_ref, out_ref.at[copy], sems.at[copy]) for copy in range(copies)
    ]
    for move in moves:
        move.start()
    for move in moves:
        move.wait()


def count_kernel(tbl_order, grp_ref, ids_ref, lengths_ref, items_ref, counts_ref, target_ref):
    history, batch = ids_ref.shape
    samples, table_rows = counts_ref.shape
    grp_count = batch // samples
    ids = ids_ref[...]
    items = items_ref[...]
    extra = jnp.concatenate(
        [
            lengths_ref[...],
            lax.shift_right_logical(items, 6),
            jnp.bitwise_and(items, 63),
            jnp.zeros((5, batch), jnp.int32),
        ],
        axis=0,
    )
    digits = jnp.concatenate(
        [lax.shift_right_logical(ids, 6), jnp.bitwise_and(ids, 63), extra], axis=0
    )
    digits = digits.astype(F32).astype(BF16)
    sample = lax.broadcasted_iota(jnp.int32, (samples, batch), 0)
    column = lax.broadcasted_iota(jnp.int32, (samples, batch), 1)
    sample = (sample + tbl_order[0]) % samples
    chosen = jnp.where(column == sample * grp_count + grp_ref[0], 1.0, 0.0).astype(BF16)
    own = lax.dot_general(chosen, digits, (((1,), (1,)), ((), ())), preferred_element_type=F32)
    own_ids = own[:, :history] * 64.0 + own[:, history : 2 * history]
    own_lengths = own[:, 2 * history : 2 * history + 1]
    own_items = own[:, 2 * history + 1 : 2 * history + 2] * 64.0 + own[:, 2 * history + 2 : 2 * history + 3]
    position = lax.broadcasted_iota(jnp.int32, (samples, history), 1).astype(F32)
    own_ids = jnp.where(position < own_lengths, own_ids, -1.0)
    lane = lax.broadcasted_iota(jnp.int32, (8, 128), 1).astype(F32)
    for first in range(0, samples, 8):
        names = [
            jnp.broadcast_to(own_ids[first : first + 8, h : h + 1], (8, 128)) for h in range(history)
        ]
        item = jnp.broadcast_to(own_items[first : first + 8], (8, 128))

        def tile(k, carry):
            row = lane + (k * 128).astype(F32)
            total = jnp.zeros((8, 128), F32)
            for h in range(history):
                total = total + jnp.where(names[h] == row, 1.0, 0.0)
            at = pl.ds(pl.multiple_of(k * 128, 128), 128)
            counts_ref[first : first + 8, at] = total
            target_ref[first : first + 8, at] = jnp.where(item == row, 1.0, 0.0)
            return carry

        lax.fori_loop(0, table_rows // 128, tile, 0, unroll=2)


def pool_kernel(grp_order, table_ref, counts_ref, target_ref, out_ref, score_ref):
    blocks, height, width = table_ref.shape
    rows = height - SCALE_ROWS
    samples = counts_ref.shape[0]

    def scales(block):
        terms = table_ref[block, rows:, :].astype(F32)
        return terms[0:1] + (terms[1:2] + terms[2:3])

    def columns(block):
        return slice(grp_order[block] * rows, (grp_order[block] + 1) * rows)

    query = jnp.zeros((samples, width), F32)
    factor = jnp.zeros((samples, rows), F32)
    for block in range(blocks):
        target = target_ref[:, columns(block)]
        query = query + jnp.dot(
            target.astype(BF16), table_ref[block, :rows, :], preferred_element_type=F32
        )
        factor = factor + target * scales(block)
    query = query.astype(BF16)
    factor = jnp.sum(factor, axis=1, keepdims=True) * (1.0 / width)
    top = jnp.full((samples, rows), -1e30, F32)
    for block in range(blocks):
        raw = lax.dot_general(
            query, table_ref[block, :rows, :], (((1,), (1,)), ((), ())), preferred_element_type=F32
        )
        score = raw * scales(block) * factor
        at = columns(block)
        score = jnp.where(counts_ref[:, at] > 0.0, score, -1e30)
        score_ref[:, at] = score
        top = jnp.maximum(top, score)
    peak = jnp.max(top, axis=1, keepdims=True)
    mass = jnp.zeros((samples, rows), F32)
    pooled = jnp.zeros((2 * samples, width), F32)
    for block in range(blocks):
        at = columns(block)
        weight = counts_ref[:, at] * jnp.exp(score_ref[:, at] - peak)
        mass = mass + weight
        scaled = weight * scales(block)
        high = scaled.astype(BF16)
        low = (scaled - high.astype(F32)).astype(BF16)
        pooled = pooled + jnp.dot(
            jnp.concatenate([high, low], axis=0),
            table_ref[block, :rows, :],
            preferred_element_type=F32,
        )
    mass = jnp.sum(mass, axis=1, keepdims=True)
    pooled = ((pooled[:samples] + pooled[samples:]) / mass).astype(out_ref.dtype)
    for part in range(width // LANES):
        out_ref[:, part, :] = pooled[:, part * LANES : (part + 1) * LANES]


def order_kernel(tbl_order, tables_ref, pooled_ref, out_ref):
    slots, parts, lanes = pooled_ref.shape
    first = tbl_order[0]
    table = lax.broadcasted_iota(jnp.int32, (slots, slots), 0)
    place = jnp.where(table == tables_ref[...], 1.0, 0.0).astype(BF16)
    for part in range(parts):
        rows = pooled_ref[:, part, :]
        rows = jnp.concatenate([rows[slots - first :], rows[: slots - first]], axis=0)
        ordered = jnp.dot(place, rows, preferred_element_type=F32).astype(BF16)
        out_ref[0, :, part * lanes : (part + 1) * lanes] = ordered


def per_device(codes, row_scales, history_lengths, history_ids, query_items, slot_tables):
    _, rows, width = codes.shape
    batch, _, history = history_ids.shape
    tbl_count = lax.axis_size("tbl")
    grp_count = lax.axis_size("grp")
    samples = batch // grp_count
    table_rows = rows * grp_count
    grp_order = rotated(grp_count, 10)
    tbl_order = rotated(tbl_count, tbl_count // 2)
    along_grp = [[t * grp_count + g for g in grp_order] for t in range(tbl_count)]
    along_tbl = [[t * grp_count + g for t in tbl_order] for g in range(grp_count)]

    def exchange(blocks, groups):
        return lax.all_to_all(
            blocks, ("tbl", "grp"), 0, 0, axis_index_groups=groups, tiled=True
        )

    packed = pl.pallas_call(
        pack_kernel,
        out_shape=jax.ShapeDtypeStruct((grp_count, rows + SCALE_ROWS, width), BF16),
        in_specs=[HBM, HBM],
        out_specs=HBM,
        scratch_shapes=[
            pltpu.VMEM((rows + SCALE_ROWS, width), BF16),
            pltpu.VMEM((1, rows), F32),
            pltpu.SemaphoreType.DMA((grp_count + 2,)),
        ],
        name="pack",
    )(codes[0], row_scales)
    table = exchange(packed, along_grp)
    grp = lax.axis_index("grp").astype(jnp.int32).reshape(1)
    counts, target = pl.pallas_call(
        functools.partial(count_kernel, tbl_order),
        out_shape=[
            jax.ShapeDtypeStruct((samples, table_rows), F32),
            jax.ShapeDtypeStruct((samples, table_rows), F32),
        ],
        in_specs=[SMEM, VMEM, VMEM, VMEM],
        out_specs=[VMEM, VMEM],
        cost_estimate=pl.CostEstimate(flops=100_000_000, bytes_accessed=1_000_000, transcendentals=0),
        compiler_params=SMALL,
        name="count",
    )(grp, history_ids[:, 0, :].T, history_lengths.T, query_items.T)
    pooled = pl.pallas_call(
        functools.partial(pool_kernel, grp_order),
        out_shape=jax.ShapeDtypeStruct((samples, width // LANES, LANES), BF16),
        in_specs=[VMEM, VMEM, VMEM],
        out_specs=VMEM,
        scratch_shapes=[pltpu.VMEM((samples, table_rows), F32)],
        compiler_params=SMALL,
        name="pool",
    )(table, counts, target)
    arrived = exchange(pooled, along_tbl)
    return pl.pallas_call(
        functools.partial(order_kernel, tbl_order),
        out_shape=jax.ShapeDtypeStruct((1, tbl_count, width), BF16),
        in_specs=[VMEM, VMEM],
        out_specs=VMEM,
        compiler_params=SMALL,
        name="order",
    )(slot_tables.reshape(1, tbl_count), arrived)


def solution(mesh):
    placed = (
        P("tbl", "grp", None),
        P("tbl", "grp"),
        P(None, "tbl"),
        P(None, "tbl", None),
        P(None, "tbl"),
        P(),
    )
    return jax.shard_map(
        per_device,
        mesh=mesh,
        in_specs=placed,
        out_specs=P(("tbl", "grp"), None, None),
        check_vma=False,
    )
```

```python
import functools

import jax
import jax.numpy as jnp
from jax import lax
from jax.experimental import pallas as pl
from jax.experimental.pallas import tpu as pltpu
from jax.sharding import PartitionSpec as P

F32 = jnp.float32
BF16 = jnp.bfloat16
VMEM = pl.BlockSpec(memory_space=pltpu.VMEM)
SMEM = pl.BlockSpec(memory_space=pltpu.SMEM)
HBM = pl.BlockSpec(memory_space=pltpu.HBM)
SMALL = pltpu.CompilerParams(vmem_limit_bytes=16 << 20)
SCALE_ROWS = 8
LANES = 128
CHIPS_X = 4
SPARE = 6


def rotated(count, first):
    return [(place + first) % count for place in range(count)]


def pack_kernel(codes_ref, scales_ref, out_ref, block_ref, scale_ref, sems):
    copies = out_ref.shape[0]
    rows, width = codes_ref.shape
    fetch = [
        pltpu.make_async_copy(codes_ref, block_ref.at[pl.ds(0, rows)], sems.at[copies]),
        pltpu.make_async_copy(scales_ref, scale_ref, sems.at[copies + 1]),
    ]
    for move in fetch:
        move.start()
    fetch[1].wait()
    scale = scale_ref[...]
    high = scale.astype(BF16)
    rest = scale - high.astype(F32)
    middle = rest.astype(BF16)
    low = (rest - middle.astype(F32)).astype(BF16)
    place = lax.broadcasted_iota(jnp.int32, (SCALE_ROWS, width), 0)
    terms = jnp.where(
        place == 0,
        high.astype(F32),
        jnp.where(place == 1, middle.astype(F32), jnp.where(place == 2, low.astype(F32), 0.0)),
    ).astype(BF16)
    block_ref[rows:, :] = terms
    fetch[0].wait()
    moves = [
        pltpu.make_async_copy(block_ref, out_ref.at[copy], sems.at[copy]) for copy in range(copies)
    ]
    for move in moves:
        move.start()
    for move in moves:
        move.wait()


def three_terms(value):
    high = value.astype(BF16).astype(F32)
    rest = value - high
    middle = rest.astype(BF16).astype(F32)
    return high, middle, rest - middle


def count_kernel(order, grp_ref, ids_ref, lengths_ref, items_ref, counts_ref, target_ref, names_ref, item_ref):
    tbl_order, y_order, x_order = order
    history, batch = ids_ref.shape
    samples, held = counts_ref.shape
    tbl_count, x_count = len(tbl_order), len(x_order)
    grp_count = batch // tbl_count
    rows = held // x_count
    grp = grp_ref[0]
    y, x = grp // x_count, grp % x_count
    ids = ids_ref[...]
    items = items_ref[...]
    extra = jnp.concatenate(
        [
            lengths_ref[...],
            lax.shift_right_logical(items, 6),
            jnp.bitwise_and(items, 63),
            jnp.zeros((5, batch), jnp.int32),
        ],
        axis=0,
    )
    digits = jnp.concatenate(
        [lax.shift_right_logical(ids, 6), jnp.bitwise_and(ids, 63), extra], axis=0
    )
    digits = digits.astype(F32).astype(BF16)
    sample = lax.broadcasted_iota(jnp.int32, (samples, batch), 0)
    column = lax.broadcasted_iota(jnp.int32, (samples, batch), 1)
    tbl_at = (sample % tbl_count + tbl_order[0]) % tbl_count
    y_at = (sample // tbl_count + y_order[0]) % len(y_order)
    chosen = jnp.where(column == tbl_at * grp_count + y_at * x_count + x, 1.0, 0.0).astype(BF16)
    own = lax.dot_general(chosen, digits, (((1,), (1,)), ((), ())), preferred_element_type=F32)

    def held_at(high, low):
        row = (high * 64.0 + low).astype(jnp.int32)
        owner = row // rows
        block = (owner % x_count - x_order[0] + x_count) % x_count
        return jnp.where(owner // x_count == y, block * rows + row % rows, -1)

    own_lengths = own[:, 2 * history : 2 * history + 1].astype(jnp.int32)
    position = lax.broadcasted_iota(jnp.int32, (samples, history), 1)
    names = held_at(own[:, :history], own[:, history : 2 * history])
    names_ref[...] = jnp.where(position < own_lengths, names, -1)
    item = held_at(
        own[:, 2 * history + 1 : 2 * history + 2], own[:, 2 * history + 2 : 2 * history + 3]
    )
    item_ref[...] = jnp.broadcast_to(item, item_ref.shape)
    lane = lax.broadcasted_iota(jnp.int32, (8, LANES), 1)

    def group(k, carry):
        at = pl.ds(pl.multiple_of(k * 8, 8), 8)
        named = names_ref[at, :]
        named = [jnp.broadcast_to(named[:, h : h + 1], (8, LANES)) for h in range(history)]
        item = item_ref[at, :]
        for first in range(0, held, LANES):
            row = lane + first
            total = jnp.zeros((8, LANES), F32)
            for h in range(history):
                total = total + jnp.where(named[h] == row, 1.0, 0.0)
            counts_ref[at, first : first + LANES] = total
            target_ref[at, first : first + LANES] = jnp.where(item == row, 1.0, 0.0)
        return carry

    lax.fori_loop(0, samples // 8, group, 0)


def query_kernel(table_ref, target_ref, out_ref):
    copies, height, width = out_ref.shape
    blocks = table_ref.shape[0]
    rows = table_ref.shape[1] - SCALE_ROWS
    samples = target_ref.shape[0]
    codes = jnp.zeros((samples, width), F32)
    terms = jnp.zeros((SCALE_ROWS, samples), F32)
    for block in range(blocks):
        target = target_ref[:, block * rows : (block + 1) * rows].astype(BF16)
        codes = codes + jnp.dot(target, table_ref[block, :rows, :], preferred_element_type=F32)
        terms = terms + lax.dot_general(
            table_ref[block, rows:, :],
            target,
            (((1,), (1,)), ((), ())),
            preferred_element_type=F32,
        )
    codes = codes.astype(BF16)
    terms = jnp.concatenate([terms, jnp.zeros((SCALE_ROWS, width - samples), F32)], axis=1)
    terms = terms.astype(BF16)
    for copy in range(copies):
        out_ref[copy, :samples, :] = codes
        out_ref[copy, samples:, :] = terms


def pool_kernel(table_ref, counts_ref, query_ref, out_ref, score_ref):
    blocks, height, width = table_ref.shape
    rows = height - SCALE_ROWS
    samples = counts_ref.shape[0]

    def scales(block):
        terms = table_ref[block, rows:, :].astype(F32)
        return terms[0:1] + (terms[1:2] + terms[2:3])

    def columns(block):
        return slice(block * rows, (block + 1) * rows)

    query = query_ref[0].astype(F32)
    for copy in range(1, query_ref.shape[0]):
        query = query + query_ref[copy].astype(F32)
    factor = query[samples:, :samples]
    factor = (factor[0:1] + (factor[1:2] + factor[2:3])) * (1.0 / width)
    factor = jnp.broadcast_to(factor, (samples, samples)).T
    factor = jnp.concatenate([factor] * (rows // samples), axis=1)
    query = query[:samples].astype(BF16)
    top = jnp.full((samples, rows), -1e30, F32)
    for block in range(blocks):
        raw = lax.dot_general(
            query, table_ref[block, :rows, :], (((1,), (1,)), ((), ())), preferred_element_type=F32
        )
        score = raw * scales(block) * factor
        score = jnp.where(counts_ref[:, columns(block)] > 0.0, score, -1e30)
        score_ref[:, columns(block)] = score
        top = jnp.maximum(top, score)
    peak = jnp.max(top, axis=1, keepdims=True)
    mass = jnp.zeros((samples, rows), F32)
    pooled = jnp.zeros((2 * samples, width), F32)
    for block in range(blocks):
        weight = counts_ref[:, columns(block)] * jnp.exp(score_ref[:, columns(block)] - peak)
        mass = mass + weight
        scaled = weight * scales(block)
        high = scaled.astype(BF16)
        low = (scaled - high.astype(F32)).astype(BF16)
        pooled = pooled + jnp.dot(
            jnp.concatenate([high, low], axis=0),
            table_ref[block, :rows, :],
            preferred_element_type=F32,
        )
    mass = jnp.sum(mass, axis=1, keepdims=True)
    pooled = pooled[:samples] + pooled[samples:]
    high = pooled.astype(BF16).astype(F32)
    low = pooled - high
    lane = lax.broadcasted_iota(jnp.int32, (samples, width), 1)
    for place, term in enumerate(three_terms(peak) + three_terms(mass)):
        low = jnp.where(lane == width - SPARE + place, term, low)
    high = high.astype(BF16)
    low = low.astype(BF16)
    parts = width // LANES
    for part in range(parts):
        out_ref[:, part, :] = high[:, part * LANES : (part + 1) * LANES]
        out_ref[:, parts + part, :] = low[:, part * LANES : (part + 1) * LANES]


def combine_kernel(order, tables_ref, got_ref, out_ref):
    tbl_order, y_order, _ = order
    slots = len(tbl_order)
    parts = got_ref.shape[1] // 2
    pieces = [got_ref[:, part, :].astype(F32) for part in range(2 * parts)]
    last = pieces[-1]
    spare = [last[:, k : k + 1] for k in range(LANES - SPARE, LANES)]
    peak = spare[0] + (spare[1] + spare[2])
    mass = spare[3] + (spare[4] + spare[5])
    lane = lax.broadcasted_iota(jnp.int32, last.shape, 1)
    pieces[-1] = jnp.where(lane < LANES - SPARE, last, 0.0)
    ranges = [slice(k * slots, (k + 1) * slots) for k in range(len(y_order))]
    top = functools.reduce(jnp.maximum, [peak[at] for at in ranges])
    shift = [jnp.exp(peak[at] - top) for at in ranges]
    whole = sum(f * mass[at] for f, at in zip(shift, ranges))
    table = lax.broadcasted_iota(jnp.int32, (slots, slots), 0)
    place = jnp.where(table == tables_ref[...], 1.0, 0.0).astype(BF16)
    first = slots - tbl_order[0]
    for part in range(parts):
        value = pieces[part] + pieces[parts + part]
        rows = sum(f * value[at] for f, at in zip(shift, ranges)) / whole
        rows = jnp.concatenate([rows[first:], rows[:first]], axis=0).astype(BF16)
        ordered = jnp.dot(place, rows, preferred_element_type=F32).astype(BF16)
        out_ref[0, :, part * LANES : (part + 1) * LANES] = ordered


def per_device(codes, row_scales, history_lengths, history_ids, query_items, slot_tables):
    _, rows, width = codes.shape
    batch, _, history = history_ids.shape
    tbl_count = lax.axis_size("tbl")
    grp_count = lax.axis_size("grp")
    x_count = CHIPS_X
    y_count = grp_count // x_count
    samples = batch // x_count
    held = rows * x_count
    tbl_order = rotated(tbl_count, tbl_count // 2)
    y_order = rotated(y_count, y_count // 2)
    x_order = rotated(x_count, x_count // 2)
    order = (tbl_order, y_order, x_order)
    tables, ys, xs = range(tbl_count), range(y_count), range(x_count)

    def device(t, y, x):
        return (t * y_count + y) * x_count + x

    along_x = [[device(t, y, x) for x in x_order] for t in tables for y in ys]
    along_y = [[device(t, y, x) for y in y_order] for t in tables for x in xs]
    to_owner = [[device(t, y, x) for y in y_order for t in tbl_order] for x in xs]

    def exchange(blocks, groups):
        return lax.all_to_all(
            blocks, ("tbl", "grp"), 0, 0, axis_index_groups=groups, tiled=True
        )

    packed = pl.pallas_call(
        pack_kernel,
        out_shape=jax.ShapeDtypeStruct((x_count, rows + SCALE_ROWS, width), BF16),
        in_specs=[HBM, HBM],
        out_specs=HBM,
        scratch_shapes=[
            pltpu.VMEM((rows + SCALE_ROWS, width), BF16),
            pltpu.VMEM((1, rows), F32),
            pltpu.SemaphoreType.DMA((x_count + 2,)),
        ],
        name="pack",
    )(codes[0], row_scales)
    table = exchange(packed, along_x)
    grp = lax.axis_index("grp").astype(jnp.int32).reshape(1)
    counts, target = pl.pallas_call(
        functools.partial(count_kernel, order),
        out_shape=[
            jax.ShapeDtypeStruct((samples, held), F32),
            jax.ShapeDtypeStruct((samples, held), F32),
        ],
        in_specs=[SMEM, VMEM, VMEM, VMEM],
        out_specs=[VMEM, VMEM],
        scratch_shapes=[
            pltpu.VMEM((samples, history), jnp.int32),
            pltpu.VMEM((samples, LANES), jnp.int32),
        ],
        cost_estimate=pl.CostEstimate(flops=100_000_000, bytes_accessed=1_000_000, transcendentals=0),
        compiler_params=SMALL,
        name="count",
    )(grp, history_ids[:, 0, :].T, history_lengths.T, query_items.T)
    masked = pl.pallas_call(
        query_kernel,
        out_shape=jax.ShapeDtypeStruct((y_count, samples + SCALE_ROWS, width), BF16),
        in_specs=[VMEM, VMEM],
        out_specs=VMEM,
        compiler_params=SMALL,
        name="query",
    )(table, target)
    query = exchange(masked, along_y)
    partial = pl.pallas_call(
        pool_kernel,
        out_shape=jax.ShapeDtypeStruct((samples, 2 * (width // LANES), LANES), BF16),
        in_specs=[VMEM, VMEM, VMEM],
        out_specs=VMEM,
        scratch_shapes=[pltpu.VMEM((samples, held), F32)],
        compiler_params=SMALL,
        name="pool",
    )(table, counts, query)
    got = exchange(partial, to_owner)
    return pl.pallas_call(
        functools.partial(combine_kernel, order),
        out_shape=jax.ShapeDtypeStruct((1, tbl_count, width), BF16),
        in_specs=[VMEM, VMEM],
        out_specs=VMEM,
        compiler_params=SMALL,
        name="combine",
    )(slot_tables.reshape(1, tbl_count), got)


def solution(mesh):
    placed = (
        P("tbl", "grp", None),
        P("tbl", "grp"),
        P(None, "tbl"),
        P(None, "tbl", None),
        P(None, "tbl"),
        P(),
    )
    return jax.shard_map(
        per_device,
        mesh=mesh,
        in_specs=placed,
        out_specs=P(("tbl", "grp"), None, None),
        check_vma=False,
    )
```

```python
import functools

import jax
import jax.numpy as jnp
from jax import lax
from jax.experimental import pallas as pl
from jax.experimental.pallas import tpu as pltpu
from jax.sharding import PartitionSpec as P

F32 = jnp.float32
BF16 = jnp.bfloat16
VMEM = pl.BlockSpec(memory_space=pltpu.VMEM)
SMEM = pl.BlockSpec(memory_space=pltpu.SMEM)
HBM = pl.BlockSpec(memory_space=pltpu.HBM)
SMALL = pltpu.CompilerParams(vmem_limit_bytes=16 << 20)
SCALE_ROWS = 8
LANES = 128
CHIPS_X = 4


def rotated(count, first):
    return [(place + first) % count for place in range(count)]


def pack_kernel(codes_ref, scales_ref, out_ref, block_ref, scale_ref, sems):
    copies = out_ref.shape[0]
    rows, width = codes_ref.shape
    fetch = [
        pltpu.make_async_copy(codes_ref, block_ref.at[pl.ds(0, rows)], sems.at[copies]),
        pltpu.make_async_copy(scales_ref, scale_ref, sems.at[copies + 1]),
    ]
    for move in fetch:
        move.start()
    fetch[1].wait()
    scale = scale_ref[...]
    high = scale.astype(BF16)
    rest = scale - high.astype(F32)
    middle = rest.astype(BF16)
    low = (rest - middle.astype(F32)).astype(BF16)
    place = lax.broadcasted_iota(jnp.int32, (SCALE_ROWS, width), 0)
    terms = jnp.where(
        place == 0,
        high.astype(F32),
        jnp.where(place == 1, middle.astype(F32), jnp.where(place == 2, low.astype(F32), 0.0)),
    ).astype(BF16)
    block_ref[rows:, :] = terms
    fetch[0].wait()
    moves = [
        pltpu.make_async_copy(block_ref, out_ref.at[copy], sems.at[copy]) for copy in range(copies)
    ]
    for move in moves:
        move.start()
    for move in moves:
        move.wait()


def count_kernel(
    order,
    grp_ref,
    ids_ref,
    lengths_ref,
    items_ref,
    tables_ref,
    counts_ref,
    target_ref,
    place_ref,
    names_ref,
    item_ref,
):
    tbl_order, y_order, x_order = order
    history, batch = ids_ref.shape
    samples, held = counts_ref.shape
    tbl_count, x_count = len(tbl_order), len(x_order)
    grp_count = batch // tbl_count
    rows = held // x_count
    grp = grp_ref[0]
    y, x = grp // x_count, grp % x_count
    ids = ids_ref[...]
    items = items_ref[...]
    extra = jnp.concatenate(
        [
            lengths_ref[...],
            lax.shift_right_logical(items, 6),
            jnp.bitwise_and(items, 63),
            jnp.zeros((5, batch), jnp.int32),
        ],
        axis=0,
    )
    digits = jnp.concatenate(
        [lax.shift_right_logical(ids, 6), jnp.bitwise_and(ids, 63), extra], axis=0
    )
    digits = digits.astype(F32).astype(BF16)
    sample = lax.broadcasted_iota(jnp.int32, (samples, batch), 0)
    column = lax.broadcasted_iota(jnp.int32, (samples, batch), 1)
    tbl_at = (sample % tbl_count + tbl_order[0]) % tbl_count
    y_at = (sample // tbl_count + y_order[0]) % len(y_order)
    chosen = jnp.where(column == tbl_at * grp_count + y_at * x_count + x, 1.0, 0.0).astype(BF16)
    own = lax.dot_general(chosen, digits, (((1,), (1,)), ((), ())), preferred_element_type=F32)

    def held_at(high, low):
        row = (high * 64.0 + low).astype(jnp.int32)
        owner = row // rows
        block = (owner % x_count - x_order[0] + x_count) % x_count
        return jnp.where(owner // x_count == y, block * rows + row % rows, -1)

    own_lengths = own[:, 2 * history : 2 * history + 1].astype(jnp.int32)
    position = lax.broadcasted_iota(jnp.int32, (samples, history), 1)
    names = held_at(own[:, :history], own[:, history : 2 * history])
    names_ref[...] = jnp.where(position < own_lengths, names, -1)
    item = held_at(
        own[:, 2 * history + 1 : 2 * history + 2], own[:, 2 * history + 2 : 2 * history + 3]
    )
    item_ref[...] = jnp.broadcast_to(item, item_ref.shape)
    lane = lax.broadcasted_iota(jnp.int32, (8, LANES), 1)

    def group(k, carry):
        at = pl.ds(pl.multiple_of(k * 8, 8), 8)
        named = names_ref[at, :]
        named = [jnp.broadcast_to(named[:, h : h + 1], (8, LANES)) for h in range(history)]
        item = item_ref[at, :]
        for first in range(0, held, LANES):
            row = lane + first
            total = jnp.zeros((8, LANES), F32)
            for h in range(history):
                total = total + jnp.where(named[h] == row, 1.0, 0.0)
            counts_ref[at, first : first + LANES] = total
            target_ref[at, first : first + LANES] = jnp.where(item == row, 1.0, 0.0)
        return carry

    lax.fori_loop(0, samples // 8, group, 0)
    table = lax.broadcasted_iota(jnp.int32, place_ref.shape, 0)
    place_ref[...] = jnp.where(table == tables_ref[...], 1.0, 0.0)


def query_kernel(table_ref, target_ref, out_ref):
    copies, height, width = out_ref.shape
    blocks = table_ref.shape[0]
    rows = table_ref.shape[1] - SCALE_ROWS
    samples = target_ref.shape[0]
    codes = jnp.zeros((samples, width), F32)
    terms = jnp.zeros((SCALE_ROWS, samples), F32)
    for block in range(blocks):
        target = target_ref[:, block * rows : (block + 1) * rows].astype(BF16)
        codes = codes + jnp.dot(target, table_ref[block, :rows, :], preferred_element_type=F32)
        terms = terms + lax.dot_general(
            table_ref[block, rows:, :],
            target,
            (((1,), (1,)), ((), ())),
            preferred_element_type=F32,
        )
    codes = codes.astype(BF16)
    terms = jnp.concatenate([terms, jnp.zeros((SCALE_ROWS, width - samples), F32)], axis=1)
    terms = terms.astype(BF16)
    for copy in range(copies):
        out_ref[copy, :samples, :] = codes
        out_ref[copy, samples:, :] = terms


def pool_kernel(table_ref, counts_ref, query_ref, out_ref, score_ref):
    blocks, height, width = table_ref.shape
    rows = height - SCALE_ROWS
    samples = counts_ref.shape[0]

    def scales(block):
        terms = table_ref[block, rows:, :].astype(F32)
        return terms[0:1] + (terms[1:2] + terms[2:3])

    def columns(block):
        return slice(block * rows, (block + 1) * rows)

    query = query_ref[0].astype(F32)
    for copy in range(1, query_ref.shape[0]):
        query = query + query_ref[copy].astype(F32)
    factor = query[samples:, :samples]
    factor = (factor[0:1] + (factor[1:2] + factor[2:3])) * (1.0 / width)
    factor = jnp.broadcast_to(factor, (samples, samples)).T
    factor = jnp.concatenate([factor] * (rows // samples), axis=1)
    query = query[:samples].astype(BF16)
    top = jnp.full((samples, rows), -1e30, F32)
    for block in range(blocks):
        raw = lax.dot_general(
            query, table_ref[block, :rows, :], (((1,), (1,)), ((), ())), preferred_element_type=F32
        )
        score = raw * scales(block) * factor
        score = jnp.where(counts_ref[:, columns(block)] > 0.0, score, -1e30)
        score_ref[:, columns(block)] = score
        top = jnp.maximum(top, score)
    peak = jnp.max(top, axis=1, keepdims=True)
    mass = jnp.zeros((samples, rows), F32)
    pooled = jnp.zeros((2 * samples, width), F32)
    for block in range(blocks):
        weight = counts_ref[:, columns(block)] * jnp.exp(score_ref[:, columns(block)] - peak)
        mass = mass + weight
        scaled = weight * scales(block)
        high = scaled.astype(BF16)
        low = (scaled - high.astype(F32)).astype(BF16)
        pooled = pooled + jnp.dot(
            jnp.concatenate([high, low], axis=0),
            table_ref[block, :rows, :],
            preferred_element_type=F32,
        )
    mass = jnp.sum(mass, axis=1, keepdims=True)
    pooled = pooled[:samples] + pooled[samples:]
    lane = lax.broadcasted_iota(jnp.int32, (samples, LANES), 1)
    last = jnp.where(lane == 0, peak, mass)
    size = out_ref.shape[1]
    for block in range(out_ref.shape[0]):
        out_ref[block, :, :width] = pooled[block * size : (block + 1) * size]
        out_ref[block, :, width:] = last[block * size : (block + 1) * size]


def merge_kernel(got_ref, out_ref):
    count = got_ref.shape[0]
    width = got_ref.shape[2] - LANES
    peaks = [got_ref[k, :, width : width + 1] for k in range(count)]
    top = functools.reduce(jnp.maximum, peaks)
    shift = [jnp.exp(peak - top) for peak in peaks]
    mass = sum(f * got_ref[k, :, width + 1 : width + 2] for k, f in enumerate(shift))
    pooled = sum(f * got_ref[k, :, :width] for k, f in enumerate(shift)) / mass
    pooled = pooled.astype(BF16)
    for part in range(width // LANES):
        out_ref[:, part, :] = pooled[:, part * LANES : (part + 1) * LANES]


def order_kernel(tbl_order, place_ref, pooled_ref, out_ref):
    slots, parts, lanes = pooled_ref.shape
    first = slots - tbl_order[0]
    place = place_ref[...].astype(BF16)
    for part in range(parts):
        rows = pooled_ref[:, part, :]
        rows = jnp.concatenate([rows[first:], rows[:first]], axis=0)
        ordered = jnp.dot(place, rows, preferred_element_type=F32).astype(BF16)
        out_ref[0, :, part * lanes : (part + 1) * lanes] = ordered


def per_device(codes, row_scales, history_lengths, history_ids, query_items, slot_tables):
    _, rows, width = codes.shape
    batch, _, history = history_ids.shape
    tbl_count = lax.axis_size("tbl")
    grp_count = lax.axis_size("grp")
    x_count = CHIPS_X
    y_count = grp_count // x_count
    samples = batch // x_count
    held = rows * x_count
    tbl_order = rotated(tbl_count, tbl_count // 2)
    y_order = rotated(y_count, y_count // 2)
    x_order = rotated(x_count, x_count // 2)
    order = (tbl_order, y_order, x_order)
    tables, ys, xs = range(tbl_count), range(y_count), range(x_count)

    def device(t, y, x):
        return (t * y_count + y) * x_count + x

    along_x = [[device(t, y, x) for x in x_order] for t in tables for y in ys]
    along_y = [[device(t, y, x) for y in y_order] for t in tables for x in xs]
    along_tbl = [[device(t, y, x) for t in tbl_order] for y in ys for x in xs]

    def exchange(blocks, groups):
        return lax.all_to_all(
            blocks, ("tbl", "grp"), 0, 0, axis_index_groups=groups, tiled=True
        )

    packed = pl.pallas_call(
        pack_kernel,
        out_shape=jax.ShapeDtypeStruct((x_count, rows + SCALE_ROWS, width), BF16),
        in_specs=[HBM, HBM],
        out_specs=HBM,
        scratch_shapes=[
            pltpu.VMEM((rows + SCALE_ROWS, width), BF16),
            pltpu.VMEM((1, rows), F32),
            pltpu.SemaphoreType.DMA((x_count + 2,)),
        ],
        name="pack",
    )(codes[0], row_scales)
    table = exchange(packed, along_x)
    grp = lax.axis_index("grp").astype(jnp.int32).reshape(1)
    counts, target, place = pl.pallas_call(
        functools.partial(count_kernel, order),
        out_shape=[
            jax.ShapeDtypeStruct((samples, held), F32),
            jax.ShapeDtypeStruct((samples, held), F32),
            jax.ShapeDtypeStruct((tbl_count, tbl_count), F32),
        ],
        in_specs=[SMEM, VMEM, VMEM, VMEM, VMEM],
        out_specs=[VMEM, VMEM, VMEM],
        scratch_shapes=[
            pltpu.VMEM((samples, history), jnp.int32),
            pltpu.VMEM((samples, LANES), jnp.int32),
        ],
        cost_estimate=pl.CostEstimate(flops=100_000_000, bytes_accessed=1_000_000, transcendentals=0),
        compiler_params=SMALL,
        name="count",
    )(
        grp,
        history_ids[:, 0, :].T,
        history_lengths.T,
        query_items.T,
        slot_tables.reshape(1, tbl_count),
    )
    masked = pl.pallas_call(
        query_kernel,
        out_shape=jax.ShapeDtypeStruct((y_count, samples + SCALE_ROWS, width), BF16),
        in_specs=[VMEM, VMEM],
        out_specs=VMEM,
        compiler_params=SMALL,
        name="query",
    )(table, target)
    query = exchange(masked, along_y)
    partial = pl.pallas_call(
        pool_kernel,
        out_shape=jax.ShapeDtypeStruct((y_count, samples // y_count, width + LANES), F32),
        in_specs=[VMEM, VMEM, VMEM],
        out_specs=VMEM,
        scratch_shapes=[pltpu.VMEM((samples, held), F32)],
        compiler_params=SMALL,
        name="pool",
    )(table, counts, query)
    got = exchange(partial, along_y)
    pooled = pl.pallas_call(
        merge_kernel,
        out_shape=jax.ShapeDtypeStruct((tbl_count, width // LANES, LANES), BF16),
        in_specs=[VMEM],
        out_specs=VMEM,
        compiler_params=SMALL,
        name="merge",
    )(got)
    arrived = exchange(pooled, along_tbl)
    return pl.pallas_call(
        functools.partial(order_kernel, tbl_order),
        out_shape=jax.ShapeDtypeStruct((1, tbl_count, width), BF16),
        in_specs=[VMEM, VMEM],
        out_specs=VMEM,
        compiler_params=SMALL,
        name="order",
    )(place, arrived)


def solution(mesh):
    placed = (
        P("tbl", "grp", None),
        P("tbl", "grp"),
        P(None, "tbl"),
        P(None, "tbl", None),
        P(None, "tbl"),
        P(),
    )
    return jax.shard_map(
        per_device,
        mesh=mesh,
        in_specs=placed,
        out_specs=P(("tbl", "grp"), None, None),
        check_vma=False,
    )
```

```python
import functools

import jax
import jax.numpy as jnp
from jax import lax
from jax.experimental import pallas as pl
from jax.experimental.pallas import tpu as pltpu
from jax.sharding import PartitionSpec as P

F32 = jnp.float32
BF16 = jnp.bfloat16
VMEM = pl.BlockSpec(memory_space=pltpu.VMEM)
SMEM = pl.BlockSpec(memory_space=pltpu.SMEM)
HBM = pl.BlockSpec(memory_space=pltpu.HBM)
SMALL = pltpu.CompilerParams(vmem_limit_bytes=16 << 20)
SCALE_ROWS = 8
LANES = 128
CHIPS_SIDE = 4


def rotated(count, first):
    return [(place + first) % count for place in range(count)]


def pack_kernel(codes_ref, scales_ref, out_ref, block_ref, scale_ref, sems):
    copies = out_ref.shape[0]
    rows, width = codes_ref.shape
    fetch = [
        pltpu.make_async_copy(codes_ref, block_ref.at[pl.ds(0, rows)], sems.at[copies]),
        pltpu.make_async_copy(scales_ref, scale_ref, sems.at[copies + 1]),
    ]
    for move in fetch:
        move.start()
    fetch[1].wait()
    scale = scale_ref[...]
    high = scale.astype(BF16)
    rest = scale - high.astype(F32)
    middle = rest.astype(BF16)
    low = (rest - middle.astype(F32)).astype(BF16)
    place = lax.broadcasted_iota(jnp.int32, (SCALE_ROWS, width), 0)
    terms = jnp.where(
        place == 0,
        high.astype(F32),
        jnp.where(place == 1, middle.astype(F32), jnp.where(place == 2, low.astype(F32), 0.0)),
    ).astype(BF16)
    block_ref[rows:, :] = terms
    fetch[0].wait()
    moves = [
        pltpu.make_async_copy(block_ref, out_ref.at[copy], sems.at[copy]) for copy in range(copies)
    ]
    for move in moves:
        move.start()
    for move in moves:
        move.wait()


def count_kernel(
    order,
    tbl_ref,
    grp_ref,
    ids_ref,
    lengths_ref,
    items_ref,
    tables_ref,
    counts_ref,
    target_ref,
    place_ref,
    names_ref,
    item_ref,
):
    tbl_order, side_order = order
    history, batch = ids_ref.shape
    samples, held = counts_ref.shape
    tbl_count, side = len(tbl_order), len(side_order)
    rows = held // side
    turned = tbl_ref[0] % 2 == 1

    def split(grp):
        y, x = grp // side, grp % side
        return jnp.where(turned, y, x), jnp.where(turned, x, y)

    along, across = split(grp_ref[0])
    ids = ids_ref[...]
    items = items_ref[...]
    extra = jnp.concatenate(
        [
            lengths_ref[...],
            lax.shift_right_logical(items, 6),
            jnp.bitwise_and(items, 63),
            jnp.zeros((5, batch), jnp.int32),
        ],
        axis=0,
    )
    digits = jnp.concatenate(
        [lax.shift_right_logical(ids, 6), jnp.bitwise_and(ids, 63), extra], axis=0
    )
    digits = digits.astype(F32).astype(BF16)
    sample = lax.broadcasted_iota(jnp.int32, (samples, batch), 0)
    column = lax.broadcasted_iota(jnp.int32, (samples, batch), 1)
    tbl_at = (sample % tbl_count + tbl_order[0]) % tbl_count
    across_at = (sample // tbl_count + side_order[0]) % side
    grp_at = jnp.where(turned, along * side + across_at, across_at * side + along)
    chosen = jnp.where(column == tbl_at * side * side + grp_at, 1.0, 0.0).astype(BF16)
    own = lax.dot_general(chosen, digits, (((1,), (1,)), ((), ())), preferred_element_type=F32)

    def held_at(high, low):
        row = (high * 64.0 + low).astype(jnp.int32)
        owner_along, owner_across = split(row // rows)
        block = (owner_along - side_order[0] + side) % side
        return jnp.where(owner_across == across, block * rows + row % rows, -1)

    own_lengths = own[:, 2 * history : 2 * history + 1].astype(jnp.int32)
    position = lax.broadcasted_iota(jnp.int32, (samples, history), 1)
    names = held_at(own[:, :history], own[:, history : 2 * history])
    names_ref[...] = jnp.where(position < own_lengths, names, -1)
    item = held_at(
        own[:, 2 * history + 1 : 2 * history + 2], own[:, 2 * history + 2 : 2 * history + 3]
    )
    item_ref[...] = jnp.broadcast_to(item, item_ref.shape)
    lane = lax.broadcasted_iota(jnp.int32, (8, LANES), 1)

    def group(k, carry):
        at = pl.ds(pl.multiple_of(k * 8, 8), 8)
        named = names_ref[at, :]
        named = [jnp.broadcast_to(named[:, h : h + 1], (8, LANES)) for h in range(history)]
        item = item_ref[at, :]
        for first in range(0, held, LANES):
            row = lane + first
            total = jnp.zeros((8, LANES), F32)
            for h in range(history):
                total = total + jnp.where(named[h] == row, 1.0, 0.0)
            counts_ref[at, first : first + LANES] = total
            target_ref[at, first : first + LANES] = jnp.where(item == row, 1.0, 0.0)
        return carry

    lax.fori_loop(0, samples // 8, group, 0)
    table = lax.broadcasted_iota(jnp.int32, place_ref.shape, 0)
    place_ref[...] = jnp.where(table == tables_ref[...], 1.0, 0.0)


def query_kernel(table_ref, target_ref, out_ref):
    copies, height, width = out_ref.shape
    blocks = table_ref.shape[0]
    rows = table_ref.shape[1] - SCALE_ROWS
    samples = target_ref.shape[0]
    codes = jnp.zeros((samples, width), F32)
    terms = jnp.zeros((SCALE_ROWS, samples), F32)
    for block in range(blocks):
        target = target_ref[:, block * rows : (block + 1) * rows].astype(BF16)
        codes = codes + jnp.dot(target, table_ref[block, :rows, :], preferred_element_type=F32)
        terms = terms + lax.dot_general(
            table_ref[block, rows:, :],
            target,
            (((1,), (1,)), ((), ())),
            preferred_element_type=F32,
        )
    codes = codes.astype(BF16)
    terms = jnp.concatenate([terms, jnp.zeros((SCALE_ROWS, width - samples), F32)], axis=1)
    terms = terms.astype(BF16)
    for copy in range(copies):
        out_ref[copy, :samples, :] = codes
        out_ref[copy, samples:, :] = terms


def pool_kernel(table_ref, counts_ref, query_ref, out_ref, score_ref):
    blocks, height, width = table_ref.shape
    rows = height - SCALE_ROWS
    samples = counts_ref.shape[0]

    def scales(block):
        terms = table_ref[block, rows:, :].astype(F32)
        return terms[0:1] + (terms[1:2] + terms[2:3])

    def columns(block):
        return slice(block * rows, (block + 1) * rows)

    query = query_ref[0].astype(F32)
    for copy in range(1, query_ref.shape[0]):
        query = query + query_ref[copy].astype(F32)
    factor = query[samples:, :samples]
    factor = (factor[0:1] + (factor[1:2] + factor[2:3])) * (1.0 / width)
    factor = jnp.broadcast_to(factor, (samples, samples)).T
    factor = jnp.concatenate([factor] * (rows // samples), axis=1)
    query = query[:samples].astype(BF16)
    top = jnp.full((samples, rows), -1e30, F32)
    for block in range(blocks):
        raw = lax.dot_general(
            query, table_ref[block, :rows, :], (((1,), (1,)), ((), ())), preferred_element_type=F32
        )
        score = raw * scales(block) * factor
        score = jnp.where(counts_ref[:, columns(block)] > 0.0, score, -1e30)
        score_ref[:, columns(block)] = score
        top = jnp.maximum(top, score)
    peak = jnp.max(top, axis=1, keepdims=True)
    mass = jnp.zeros((samples, rows), F32)
    pooled = jnp.zeros((2 * samples, width), F32)
    for block in range(blocks):
        weight = counts_ref[:, columns(block)] * jnp.exp(score_ref[:, columns(block)] - peak)
        mass = mass + weight
        scaled = weight * scales(block)
        high = scaled.astype(BF16)
        low = (scaled - high.astype(F32)).astype(BF16)
        pooled = pooled + jnp.dot(
            jnp.concatenate([high, low], axis=0),
            table_ref[block, :rows, :],
            preferred_element_type=F32,
        )
    mass = jnp.sum(mass, axis=1, keepdims=True)
    pooled = pooled[:samples] + pooled[samples:]
    lane = lax.broadcasted_iota(jnp.int32, (samples, LANES), 1)
    last = jnp.where(lane == 0, peak, mass)
    size = out_ref.shape[1]
    for block in range(out_ref.shape[0]):
        out_ref[block, :, :width] = pooled[block * size : (block + 1) * size]
        out_ref[block, :, width:] = last[block * size : (block + 1) * size]


def merge_kernel(got_ref, out_ref):
    count = got_ref.shape[0]
    width = got_ref.shape[2] - LANES
    peaks = [got_ref[k, :, width : width + 1] for k in range(count)]
    top = functools.reduce(jnp.maximum, peaks)
    shift = [jnp.exp(peak - top) for peak in peaks]
    mass = sum(f * got_ref[k, :, width + 1 : width + 2] for k, f in enumerate(shift))
    pooled = sum(f * got_ref[k, :, :width] for k, f in enumerate(shift)) / mass
    pooled = pooled.astype(BF16)
    for part in range(width // LANES):
        out_ref[:, part, :] = pooled[:, part * LANES : (part + 1) * LANES]


def order_kernel(tbl_order, place_ref, pooled_ref, out_ref):
    slots, parts, lanes = pooled_ref.shape
    first = slots - tbl_order[0]
    place = place_ref[...].astype(BF16)
    for part in range(parts):
        rows = pooled_ref[:, part, :]
        rows = jnp.concatenate([rows[first:], rows[:first]], axis=0)
        ordered = jnp.dot(place, rows, preferred_element_type=F32).astype(BF16)
        out_ref[0, :, part * lanes : (part + 1) * lanes] = ordered


def per_device(codes, row_scales, history_lengths, history_ids, query_items, slot_tables):
    _, rows, width = codes.shape
    batch, _, history = history_ids.shape
    tbl_count = lax.axis_size("tbl")
    grp_count = lax.axis_size("grp")
    side = CHIPS_SIDE
    samples = tbl_count * side
    held = rows * side
    tbl_order = rotated(tbl_count, tbl_count // 2 + 1)
    side_order = rotated(side, side // 2)
    order = (tbl_order, side_order)
    tables, places = range(tbl_count), range(side)

    def device(t, along, across):
        y, x = (along, across) if t % 2 else (across, along)
        return (t * side + y) * side + x

    along_rows = [[device(t, u, v) for u in side_order] for t in tables for v in places]
    across_rows = [[device(t, u, v) for v in side_order] for t in tables for u in places]
    along_tbl = [[t * grp_count + g for t in tbl_order] for g in range(grp_count)]

    def exchange(blocks, groups):
        return lax.all_to_all(
            blocks, ("tbl", "grp"), 0, 0, axis_index_groups=groups, tiled=True
        )

    packed = pl.pallas_call(
        pack_kernel,
        out_shape=jax.ShapeDtypeStruct((side, rows + SCALE_ROWS, width), BF16),
        in_specs=[HBM, HBM],
        out_specs=HBM,
        scratch_shapes=[
            pltpu.VMEM((rows + SCALE_ROWS, width), BF16),
            pltpu.VMEM((1, rows), F32),
            pltpu.SemaphoreType.DMA((side + 2,)),
        ],
        name="pack",
    )(codes[0], row_scales)
    table = exchange(packed, along_rows)
    tbl = lax.axis_index("tbl").astype(jnp.int32).reshape(1)
    grp = lax.axis_index("grp").astype(jnp.int32).reshape(1)
    counts, target, place = pl.pallas_call(
        functools.partial(count_kernel, order),
        out_shape=[
            jax.ShapeDtypeStruct((samples, held), F32),
            jax.ShapeDtypeStruct((samples, held), F32),
            jax.ShapeDtypeStruct((tbl_count, tbl_count), F32),
        ],
        in_specs=[SMEM, SMEM, VMEM, VMEM, VMEM, VMEM],
        out_specs=[VMEM, VMEM, VMEM],
        scratch_shapes=[
            pltpu.VMEM((samples, history), jnp.int32),
            pltpu.VMEM((samples, LANES), jnp.int32),
        ],
        cost_estimate=pl.CostEstimate(flops=100_000_000, bytes_accessed=1_000_000, transcendentals=0),
        compiler_params=SMALL,
        name="count",
    )(
        tbl,
        grp,
        history_ids[:, 0, :].T,
        history_lengths.T,
        query_items.T,
        slot_tables.reshape(1, tbl_count),
    )
    masked = pl.pallas_call(
        query_kernel,
        out_shape=jax.ShapeDtypeStruct((side, samples + SCALE_ROWS, width), BF16),
        in_specs=[VMEM, VMEM],
        out_specs=VMEM,
        compiler_params=SMALL,
        name="query",
    )(table, target)
    query = exchange(masked, across_rows)
    partial = pl.pallas_call(
        pool_kernel,
        out_shape=jax.ShapeDtypeStruct((side, samples // side, width + LANES), F32),
        in_specs=[VMEM, VMEM, VMEM],
        out_specs=VMEM,
        scratch_shapes=[pltpu.VMEM((samples, held), F32)],
        compiler_params=SMALL,
        name="pool",
    )(table, counts, query)
    got = exchange(partial, across_rows)
    pooled = pl.pallas_call(
        merge_kernel,
        out_shape=jax.ShapeDtypeStruct((tbl_count, width // LANES, LANES), BF16),
        in_specs=[VMEM],
        out_specs=VMEM,
        compiler_params=SMALL,
        name="merge",
    )(got)
    arrived = exchange(pooled, along_tbl)
    return pl.pallas_call(
        functools.partial(order_kernel, tbl_order),
        out_shape=jax.ShapeDtypeStruct((1, tbl_count, width), BF16),
        in_specs=[VMEM, VMEM],
        out_specs=VMEM,
        compiler_params=SMALL,
        name="order",
    )(place, arrived)


def solution(mesh):
    placed = (
        P("tbl", "grp", None),
        P("tbl", "grp"),
        P(None, "tbl"),
        P(None, "tbl", None),
        P(None, "tbl"),
        P(),
    )
    return jax.shard_map(
        per_device,
        mesh=mesh,
        in_specs=placed,
        out_specs=P(("tbl", "grp"), None, None),
        check_vma=False,
    )
```

```python
import functools

import jax
import jax.numpy as jnp
from jax import lax
from jax.experimental import pallas as pl
from jax.experimental.pallas import tpu as pltpu
from jax.sharding import PartitionSpec as P

F32 = jnp.float32
BF16 = jnp.bfloat16
VMEM = pl.BlockSpec(memory_space=pltpu.VMEM)
SMEM = pl.BlockSpec(memory_space=pltpu.SMEM)
HBM = pl.BlockSpec(memory_space=pltpu.HBM)
SMALL = pltpu.CompilerParams(vmem_limit_bytes=16 << 20)
SCALE_ROWS = 8
LANES = 128
CHIPS_SIDE = 4


def rotated(count, first):
    return [(place + first) % count for place in range(count)]


def pack_kernel(codes_ref, scales_ref, out_ref, block_ref, scale_ref, sems):
    copies = out_ref.shape[0]
    rows, width = codes_ref.shape
    fetch = [
        pltpu.make_async_copy(codes_ref, block_ref.at[pl.ds(0, rows)], sems.at[copies]),
        pltpu.make_async_copy(scales_ref, scale_ref, sems.at[copies + 1]),
    ]
    for move in fetch:
        move.start()
    fetch[1].wait()
    scale = scale_ref[...]
    high = scale.astype(BF16)
    rest = scale - high.astype(F32)
    middle = rest.astype(BF16)
    low = (rest - middle.astype(F32)).astype(BF16)
    place = lax.broadcasted_iota(jnp.int32, (SCALE_ROWS, width), 0)
    terms = jnp.where(
        place == 0,
        high.astype(F32),
        jnp.where(place == 1, middle.astype(F32), jnp.where(place == 2, low.astype(F32), 0.0)),
    ).astype(BF16)
    block_ref[rows:, :] = terms
    fetch[0].wait()
    moves = [
        pltpu.make_async_copy(block_ref, out_ref.at[copy], sems.at[copy]) for copy in range(copies)
    ]
    for move in moves:
        move.start()
    for move in moves:
        move.wait()


def count_kernel(
    order,
    tbl_ref,
    grp_ref,
    ids_ref,
    lengths_ref,
    items_ref,
    tables_ref,
    counts_ref,
    target_ref,
    place_ref,
    names_ref,
    item_ref,
):
    tbl_order, side_order = order
    history, batch = ids_ref.shape
    samples, held = counts_ref.shape
    tbl_count, side = len(tbl_order), len(side_order)
    rows = held // side
    turned = tbl_ref[0] % 2 == 0

    def split(grp):
        y, x = grp // side, grp % side
        return jnp.where(turned, y, x), jnp.where(turned, x, y)

    along, across = split(grp_ref[0])
    ids = ids_ref[...]
    items = items_ref[...]
    extra = jnp.concatenate(
        [
            lengths_ref[...],
            lax.shift_right_logical(items, 6),
            jnp.bitwise_and(items, 63),
            jnp.zeros((5, batch), jnp.int32),
        ],
        axis=0,
    )
    digits = jnp.concatenate(
        [lax.shift_right_logical(ids, 6), jnp.bitwise_and(ids, 63), extra], axis=0
    )
    digits = digits.astype(F32).astype(BF16)
    sample = lax.broadcasted_iota(jnp.int32, (samples, batch), 0)
    column = lax.broadcasted_iota(jnp.int32, (samples, batch), 1)
    tbl_at = (sample % tbl_count + tbl_order[0]) % tbl_count
    across_at = (sample // tbl_count + side_order[0]) % side
    grp_at = jnp.where(turned, along * side + across_at, across_at * side + along)
    chosen = jnp.where(column == tbl_at * side * side + grp_at, 1.0, 0.0).astype(BF16)
    own = lax.dot_general(chosen, digits, (((1,), (1,)), ((), ())), preferred_element_type=F32)

    def held_at(high, low):
        row = (high * 64.0 + low).astype(jnp.int32)
        owner_along, owner_across = split(row // rows)
        block = (owner_along - side_order[0] + side) % side
        return jnp.where(owner_across == across, block * rows + row % rows, -1)

    own_lengths = own[:, 2 * history : 2 * history + 1].astype(jnp.int32)
    position = lax.broadcasted_iota(jnp.int32, (samples, history), 1)
    names = held_at(own[:, :history], own[:, history : 2 * history])
    names_ref[...] = jnp.where(position < own_lengths, names, -1)
    item = held_at(
        own[:, 2 * history + 1 : 2 * history + 2], own[:, 2 * history + 2 : 2 * history + 3]
    )
    item_ref[...] = jnp.broadcast_to(item, item_ref.shape)
    lane = lax.broadcasted_iota(jnp.int32, (16, LANES), 1)
    one = jnp.ones((16, LANES), BF16)
    none = jnp.zeros((16, LANES), BF16)

    def group(k, carry):
        at = pl.ds(pl.multiple_of(k * 16, 16), 16)
        named = names_ref[at, :]
        named = [
            jnp.broadcast_to(named[:, h : h + 1], (16, LANES)).astype(jnp.int16)
            for h in range(history)
        ]
        item = item_ref[at, :]
        for first in range(0, held, LANES):
            row = (lane + first).astype(jnp.int16)
            total = none
            for h in range(history):
                total = total + jnp.where(named[h] == row, one, none)
            counts_ref[at, first : first + LANES] = total.astype(F32)
            target_ref[at, first : first + LANES] = jnp.where(item == lane + first, 1.0, 0.0)
        return carry

    lax.fori_loop(0, samples // 16, group, 0)
    table = lax.broadcasted_iota(jnp.int32, place_ref.shape, 0)
    place_ref[...] = jnp.where(table == tables_ref[...], 1.0, 0.0)


def query_kernel(table_ref, target_ref, out_ref):
    copies, height, width = out_ref.shape
    blocks = table_ref.shape[0]
    rows = table_ref.shape[1] - SCALE_ROWS
    samples = target_ref.shape[0]
    codes = jnp.zeros((samples, width), F32)
    terms = jnp.zeros((SCALE_ROWS, samples), F32)
    for block in range(blocks):
        target = target_ref[:, block * rows : (block + 1) * rows].astype(BF16)
        codes = codes + jnp.dot(target, table_ref[block, :rows, :], preferred_element_type=F32)
        terms = terms + lax.dot_general(
            table_ref[block, rows:, :],
            target,
            (((1,), (1,)), ((), ())),
            preferred_element_type=F32,
        )
    codes = codes.astype(BF16)
    terms = jnp.concatenate([terms, jnp.zeros((SCALE_ROWS, width - samples), F32)], axis=1)
    terms = terms.astype(BF16)
    for copy in range(copies):
        out_ref[copy, :samples, :] = codes
        out_ref[copy, samples:, :] = terms


def pool_kernel(table_ref, counts_ref, query_ref, out_ref, score_ref):
    blocks, height, width = table_ref.shape
    rows = height - SCALE_ROWS
    samples = counts_ref.shape[0]

    def scales(block):
        terms = table_ref[block, rows:, :].astype(F32)
        return terms[0:1] + (terms[1:2] + terms[2:3])

    def columns(block):
        return slice(block * rows, (block + 1) * rows)

    query = query_ref[0].astype(F32)
    for copy in range(1, query_ref.shape[0]):
        query = query + query_ref[copy].astype(F32)
    factor = query[samples:, :samples]
    factor = (factor[0:1] + (factor[1:2] + factor[2:3])) * (1.0 / width)
    factor = jnp.broadcast_to(factor, (samples, samples)).T
    factor = jnp.concatenate([factor] * (rows // samples), axis=1)
    query = query[:samples].astype(BF16)
    top = jnp.full((samples, rows), -1e30, F32)
    for block in range(blocks):
        raw = lax.dot_general(
            query, table_ref[block, :rows, :], (((1,), (1,)), ((), ())), preferred_element_type=F32
        )
        score = raw * scales(block) * factor
        score = jnp.where(counts_ref[:, columns(block)] > 0.0, score, -1e30)
        score_ref[:, columns(block)] = score
        top = jnp.maximum(top, score)
    peak = jnp.max(top, axis=1, keepdims=True)
    mass = jnp.zeros((samples, rows), F32)
    pooled = jnp.zeros((2 * samples, width), F32)
    for block in range(blocks):
        weight = counts_ref[:, columns(block)] * jnp.exp(score_ref[:, columns(block)] - peak)
        mass = mass + weight
        scaled = weight * scales(block)
        high = scaled.astype(BF16)
        low = (scaled - high.astype(F32)).astype(BF16)
        pooled = pooled + jnp.dot(
            jnp.concatenate([high, low], axis=0),
            table_ref[block, :rows, :],
            preferred_element_type=F32,
        )
    mass = jnp.sum(mass, axis=1, keepdims=True)
    pooled = pooled[:samples] + pooled[samples:]
    lane = lax.broadcasted_iota(jnp.int32, (samples, LANES), 1)
    last = jnp.where(lane == 0, peak, mass)
    size = out_ref.shape[1]
    for block in range(out_ref.shape[0]):
        out_ref[block, :, :width] = pooled[block * size : (block + 1) * size]
        out_ref[block, :, width:] = last[block * size : (block + 1) * size]


def merge_kernel(got_ref, out_ref):
    count = got_ref.shape[0]
    width = got_ref.shape[2] - LANES
    peaks = [got_ref[k, :, width : width + 1] for k in range(count)]
    top = functools.reduce(jnp.maximum, peaks)
    shift = [jnp.exp(peak - top) for peak in peaks]
    mass = sum(f * got_ref[k, :, width + 1 : width + 2] for k, f in enumerate(shift))
    pooled = sum(f * got_ref[k, :, :width] for k, f in enumerate(shift)) / mass
    pooled = pooled.astype(BF16)
    for part in range(width // LANES):
        out_ref[:, part, :] = pooled[:, part * LANES : (part + 1) * LANES]


def order_kernel(tbl_order, place_ref, pooled_ref, out_ref):
    slots, parts, lanes = pooled_ref.shape
    first = slots - tbl_order[0]
    place = place_ref[...].astype(BF16)
    for part in range(parts):
        rows = pooled_ref[:, part, :]
        rows = jnp.concatenate([rows[first:], rows[:first]], axis=0)
        ordered = jnp.dot(place, rows, preferred_element_type=F32).astype(BF16)
        out_ref[0, :, part * lanes : (part + 1) * lanes] = ordered


def per_device(codes, row_scales, history_lengths, history_ids, query_items, slot_tables):
    _, rows, width = codes.shape
    batch, _, history = history_ids.shape
    tbl_count = lax.axis_size("tbl")
    grp_count = lax.axis_size("grp")
    side = CHIPS_SIDE
    samples = tbl_count * side
    held = rows * side
    tbl_order = rotated(tbl_count, tbl_count // 2 + 3)
    side_order = rotated(side, side // 2)
    order = (tbl_order, side_order)
    tables, places = range(tbl_count), range(side)

    def device(t, along, across):
        y, x = (across, along) if t % 2 else (along, across)
        return (t * side + y) * side + x

    along_rows = [[device(t, u, v) for u in side_order] for t in tables for v in places]
    across_rows = [[device(t, u, v) for v in side_order] for t in tables for u in places]
    along_tbl = [[t * grp_count + g for t in tbl_order] for g in range(grp_count)]

    def exchange(blocks, groups):
        return lax.all_to_all(
            blocks, ("tbl", "grp"), 0, 0, axis_index_groups=groups, tiled=True
        )

    packed = pl.pallas_call(
        pack_kernel,
        out_shape=jax.ShapeDtypeStruct((side, rows + SCALE_ROWS, width), BF16),
        in_specs=[HBM, HBM],
        out_specs=HBM,
        scratch_shapes=[
            pltpu.VMEM((rows + SCALE_ROWS, width), BF16),
            pltpu.VMEM((1, rows), F32),
            pltpu.SemaphoreType.DMA((side + 2,)),
        ],
        name="pack",
    )(codes[0], row_scales)
    table = exchange(packed, along_rows)
    tbl = lax.axis_index("tbl").astype(jnp.int32).reshape(1)
    grp = lax.axis_index("grp").astype(jnp.int32).reshape(1)
    counts, target, place = pl.pallas_call(
        functools.partial(count_kernel, order),
        out_shape=[
            jax.ShapeDtypeStruct((samples, held), F32),
            jax.ShapeDtypeStruct((samples, held), F32),
            jax.ShapeDtypeStruct((tbl_count, tbl_count), F32),
        ],
        in_specs=[SMEM, SMEM, VMEM, VMEM, VMEM, VMEM],
        out_specs=[VMEM, VMEM, VMEM],
        scratch_shapes=[
            pltpu.VMEM((samples, history), jnp.int32),
            pltpu.VMEM((samples, LANES), jnp.int32),
        ],
        cost_estimate=pl.CostEstimate(flops=100_000_000, bytes_accessed=1_000_000, transcendentals=0),
        compiler_params=SMALL,
        name="count",
    )(
        tbl,
        grp,
        history_ids[:, 0, :].T,
        history_lengths.T,
        query_items.T,
        slot_tables.reshape(1, tbl_count),
    )
    masked = pl.pallas_call(
        query_kernel,
        out_shape=jax.ShapeDtypeStruct((side, samples + SCALE_ROWS, width), BF16),
        in_specs=[VMEM, VMEM],
        out_specs=VMEM,
        compiler_params=SMALL,
        name="query",
    )(table, target)
    query = exchange(masked, across_rows)
    partial = pl.pallas_call(
        pool_kernel,
        out_shape=jax.ShapeDtypeStruct((side, samples // side, width + LANES), F32),
        in_specs=[VMEM, VMEM, VMEM],
        out_specs=VMEM,
        scratch_shapes=[pltpu.VMEM((samples, held), F32)],
        compiler_params=SMALL,
        name="pool",
    )(table, counts, query)
    got = exchange(partial, across_rows)
    pooled = pl.pallas_call(
        merge_kernel,
        out_shape=jax.ShapeDtypeStruct((tbl_count, width // LANES, LANES), BF16),
        in_specs=[VMEM],
        out_specs=VMEM,
        compiler_params=SMALL,
        name="merge",
    )(got)
    arrived = exchange(pooled, along_tbl)
    return pl.pallas_call(
        functools.partial(order_kernel, tbl_order),
        out_shape=jax.ShapeDtypeStruct((1, tbl_count, width), BF16),
        in_specs=[VMEM, VMEM],
        out_specs=VMEM,
        compiler_params=SMALL,
        name="order",
    )(place, arrived)


def solution(mesh):
    placed = (
        P("tbl", "grp", None),
        P("tbl", "grp"),
        P(None, "tbl"),
        P(None, "tbl", None),
        P(None, "tbl"),
        P(),
    )
    return jax.shard_map(
        per_device,
        mesh=mesh,
        in_specs=placed,
        out_specs=P(("tbl", "grp"), None, None),
        check_vma=False,
    )
```

```python
import functools

import jax
import jax.numpy as jnp
from jax import lax
from jax.experimental import pallas as pl
from jax.experimental.pallas import tpu as pltpu
from jax.sharding import PartitionSpec as P

F32 = jnp.float32
BF16 = jnp.bfloat16
VMEM = pl.BlockSpec(memory_space=pltpu.VMEM)
SMEM = pl.BlockSpec(memory_space=pltpu.SMEM)
HBM = pl.BlockSpec(memory_space=pltpu.HBM)
SMALL = pltpu.CompilerParams(vmem_limit_bytes=16 << 20)
SCALE_ROWS = 8
LANES = 128
CHIPS_SIDE = 4
SPARE = 6


def rotated(count, first):
    return [(place + first) % count for place in range(count)]


def pack_kernel(codes_ref, scales_ref, out_ref, block_ref, scale_ref, sems):
    copies = out_ref.shape[0]
    rows, width = codes_ref.shape
    fetch = [
        pltpu.make_async_copy(codes_ref, block_ref.at[pl.ds(0, rows)], sems.at[copies]),
        pltpu.make_async_copy(scales_ref, scale_ref, sems.at[copies + 1]),
    ]
    for move in fetch:
        move.start()
    fetch[1].wait()
    scale = scale_ref[...]
    high = scale.astype(BF16)
    rest = scale - high.astype(F32)
    middle = rest.astype(BF16)
    low = (rest - middle.astype(F32)).astype(BF16)
    place = lax.broadcasted_iota(jnp.int32, (SCALE_ROWS, width), 0)
    terms = jnp.where(
        place == 0,
        high.astype(F32),
        jnp.where(place == 1, middle.astype(F32), jnp.where(place == 2, low.astype(F32), 0.0)),
    ).astype(BF16)
    block_ref[rows:, :] = terms
    fetch[0].wait()
    moves = [
        pltpu.make_async_copy(block_ref, out_ref.at[copy], sems.at[copy]) for copy in range(copies)
    ]
    for move in moves:
        move.start()
    for move in moves:
        move.wait()


def three_terms(value):
    high = value.astype(BF16).astype(F32)
    rest = value - high
    middle = rest.astype(BF16).astype(F32)
    return high, middle, rest - middle


def count_kernel(
    order,
    tbl_ref,
    grp_ref,
    ids_ref,
    lengths_ref,
    items_ref,
    tables_ref,
    counts_ref,
    target_ref,
    place_ref,
    names_ref,
    item_ref,
):
    tbl_order, side_order = order
    history, batch = ids_ref.shape
    samples, held = counts_ref.shape
    tbl_count, side = len(tbl_order), len(side_order)
    rows = held // side
    turned = tbl_ref[0] % 2 == 0

    def split(grp):
        y, x = grp // side, grp % side
        return jnp.where(turned, y, x), jnp.where(turned, x, y)

    along, across = split(grp_ref[0])
    ids = ids_ref[...]
    items = items_ref[...]
    extra = jnp.concatenate(
        [
            lengths_ref[...],
            lax.shift_right_logical(items, 6),
            jnp.bitwise_and(items, 63),
            jnp.zeros((5, batch), jnp.int32),
        ],
        axis=0,
    )
    digits = jnp.concatenate(
        [lax.shift_right_logical(ids, 6), jnp.bitwise_and(ids, 63), extra], axis=0
    )
    digits = digits.astype(F32).astype(BF16)
    sample = lax.broadcasted_iota(jnp.int32, (samples, batch), 0)
    column = lax.broadcasted_iota(jnp.int32, (samples, batch), 1)
    tbl_at = (sample % tbl_count + tbl_order[0]) % tbl_count
    across_at = (sample // tbl_count + side_order[0]) % side
    grp_at = jnp.where(turned, along * side + across_at, across_at * side + along)
    chosen = jnp.where(column == tbl_at * side * side + grp_at, 1.0, 0.0).astype(BF16)
    own = lax.dot_general(chosen, digits, (((1,), (1,)), ((), ())), preferred_element_type=F32)

    def held_at(high, low):
        row = (high * 64.0 + low).astype(jnp.int32)
        owner_along, owner_across = split(row // rows)
        block = (owner_along - side_order[0] + side) % side
        return jnp.where(owner_across == across, block * rows + row % rows, -1)

    own_lengths = own[:, 2 * history : 2 * history + 1].astype(jnp.int32)
    position = lax.broadcasted_iota(jnp.int32, (samples, history), 1)
    names = held_at(own[:, :history], own[:, history : 2 * history])
    names_ref[...] = jnp.where(position < own_lengths, names, -1)
    item = held_at(
        own[:, 2 * history + 1 : 2 * history + 2], own[:, 2 * history + 2 : 2 * history + 3]
    )
    item_ref[...] = jnp.broadcast_to(item, item_ref.shape)
    lane = lax.broadcasted_iota(jnp.int32, (16, LANES), 1)
    one = jnp.ones((16, LANES), BF16)
    none = jnp.zeros((16, LANES), BF16)

    def group(k, carry):
        at = pl.ds(pl.multiple_of(k * 16, 16), 16)
        named = names_ref[at, :]
        named = [
            jnp.broadcast_to(named[:, h : h + 1], (16, LANES)).astype(jnp.int16)
            for h in range(history)
        ]
        item = item_ref[at, :]
        for first in range(0, held, LANES):
            row = (lane + first).astype(jnp.int16)
            total = none
            for h in range(history):
                total = total + jnp.where(named[h] == row, one, none)
            counts_ref[at, first : first + LANES] = total.astype(F32)
            target_ref[at, first : first + LANES] = jnp.where(item == lane + first, 1.0, 0.0)
        return carry

    lax.fori_loop(0, samples // 16, group, 0)
    table = lax.broadcasted_iota(jnp.int32, place_ref.shape, 0)
    place_ref[...] = jnp.where(table == tables_ref[...], 1.0, 0.0)


def query_kernel(table_ref, target_ref, out_ref):
    copies, height, width = out_ref.shape
    blocks = table_ref.shape[0]
    rows = table_ref.shape[1] - SCALE_ROWS
    samples = target_ref.shape[0]
    codes = jnp.zeros((samples, width), F32)
    terms = jnp.zeros((SCALE_ROWS, samples), F32)
    for block in range(blocks):
        target = target_ref[:, block * rows : (block + 1) * rows].astype(BF16)
        codes = codes + jnp.dot(target, table_ref[block, :rows, :], preferred_element_type=F32)
        terms = terms + lax.dot_general(
            table_ref[block, rows:, :],
            target,
            (((1,), (1,)), ((), ())),
            preferred_element_type=F32,
        )
    codes = codes.astype(BF16)
    terms = jnp.concatenate([terms, jnp.zeros((SCALE_ROWS, width - samples), F32)], axis=1)
    terms = terms.astype(BF16)
    for copy in range(copies):
        out_ref[copy, :samples, :] = codes
        out_ref[copy, samples:, :] = terms


def pool_kernel(table_ref, counts_ref, query_ref, out_ref, score_ref):
    blocks, height, width = table_ref.shape
    rows = height - SCALE_ROWS
    samples = counts_ref.shape[0]

    def scales(block):
        terms = table_ref[block, rows:, :].astype(F32)
        return terms[0:1] + (terms[1:2] + terms[2:3])

    def columns(block):
        return slice(block * rows, (block + 1) * rows)

    query = query_ref[0].astype(F32)
    for copy in range(1, query_ref.shape[0]):
        query = query + query_ref[copy].astype(F32)
    factor = query[samples:, :samples]
    factor = (factor[0:1] + (factor[1:2] + factor[2:3])) * (1.0 / width)
    factor = jnp.broadcast_to(factor, (samples, samples)).T
    factor = jnp.concatenate([factor] * (rows // samples), axis=1)
    query = query[:samples].astype(BF16)
    top = jnp.full((samples, rows), -1e30, F32)
    for block in range(blocks):
        raw = lax.dot_general(
            query, table_ref[block, :rows, :], (((1,), (1,)), ((), ())), preferred_element_type=F32
        )
        score = raw * scales(block) * factor
        score = jnp.where(counts_ref[:, columns(block)] > 0.0, score, -1e30)
        score_ref[:, columns(block)] = score
        top = jnp.maximum(top, score)
    peak = jnp.max(top, axis=1, keepdims=True)
    mass = jnp.zeros((samples, rows), F32)
    pooled = jnp.zeros((2 * samples, width), F32)
    for block in range(blocks):
        weight = counts_ref[:, columns(block)] * jnp.exp(score_ref[:, columns(block)] - peak)
        mass = mass + weight
        scaled = weight * scales(block)
        high = scaled.astype(BF16)
        low = (scaled - high.astype(F32)).astype(BF16)
        pooled = pooled + jnp.dot(
            jnp.concatenate([high, low], axis=0),
            table_ref[block, :rows, :],
            preferred_element_type=F32,
        )
    mass = jnp.sum(mass, axis=1, keepdims=True)
    pooled = pooled[:samples] + pooled[samples:]
    high = pooled.astype(BF16)
    low = pooled - high.astype(F32)
    lane = lax.broadcasted_iota(jnp.int32, (samples, width), 1)
    for place, term in enumerate(three_terms(peak) + three_terms(mass)):
        low = jnp.where(lane == width - SPARE + place, term, low)
    low = low.astype(BF16)
    size = out_ref.shape[1] // 2
    for block in range(out_ref.shape[0]):
        out_ref[block, :size, :] = high[block * size : (block + 1) * size]
        out_ref[block, size:, :] = low[block * size : (block + 1) * size]


def merge_kernel(got_ref, out_ref):
    count, height, width = got_ref.shape
    size = height // 2
    lane = lax.broadcasted_iota(jnp.int32, (size, width), 1)
    sums, peaks, masses = [], [], []
    for k in range(count):
        low = got_ref[k, size:, :].astype(F32)
        spare = [low[:, at : at + 1] for at in range(width - SPARE, width)]
        peaks.append(spare[0] + (spare[1] + spare[2]))
        masses.append(spare[3] + (spare[4] + spare[5]))
        low = jnp.where(lane < width - SPARE, low, 0.0)
        sums.append(got_ref[k, :size, :].astype(F32) + low)
    top = functools.reduce(jnp.maximum, peaks)
    shift = [jnp.exp(peak - top) for peak in peaks]
    mass = sum(f * part for f, part in zip(shift, masses))
    pooled = sum(f * part for f, part in zip(shift, sums)) / mass
    pooled = pooled.astype(BF16)
    for part in range(width // LANES):
        out_ref[:, part, :] = pooled[:, part * LANES : (part + 1) * LANES]


def order_kernel(tbl_order, place_ref, pooled_ref, out_ref):
    slots, parts, lanes = pooled_ref.shape
    first = slots - tbl_order[0]
    place = place_ref[...].astype(BF16)
    for part in range(parts):
        rows = pooled_ref[:, part, :]
        rows = jnp.concatenate([rows[first:], rows[:first]], axis=0)
        ordered = jnp.dot(place, rows, preferred_element_type=F32).astype(BF16)
        out_ref[0, :, part * lanes : (part + 1) * lanes] = ordered


def per_device(codes, row_scales, history_lengths, history_ids, query_items, slot_tables):
    _, rows, width = codes.shape
    batch, _, history = history_ids.shape
    tbl_count = lax.axis_size("tbl")
    grp_count = lax.axis_size("grp")
    side = CHIPS_SIDE
    samples = tbl_count * side
    held = rows * side
    tbl_order = rotated(tbl_count, tbl_count // 2 + 3)
    side_order = rotated(side, side // 2)
    order = (tbl_order, side_order)
    tables, places = range(tbl_count), range(side)

    def device(t, along, across):
        y, x = (across, along) if t % 2 else (along, across)
        return (t * side + y) * side + x

    along_rows = [[device(t, u, v) for u in side_order] for t in tables for v in places]
    across_rows = [[device(t, u, v) for v in side_order] for t in tables for u in places]
    along_tbl = [[t * grp_count + g for t in tbl_order] for g in range(grp_count)]

    def exchange(blocks, groups):
        return lax.all_to_all(
            blocks, ("tbl", "grp"), 0, 0, axis_index_groups=groups, tiled=True
        )

    packed = pl.pallas_call(
        pack_kernel,
        out_shape=jax.ShapeDtypeStruct((side, rows + SCALE_ROWS, width), BF16),
        in_specs=[HBM, HBM],
        out_specs=HBM,
        scratch_shapes=[
            pltpu.VMEM((rows + SCALE_ROWS, width), BF16),
            pltpu.VMEM((1, rows), F32),
            pltpu.SemaphoreType.DMA((side + 2,)),
        ],
        name="pack",
    )(codes[0], row_scales)
    table = exchange(packed, along_rows)
    tbl = lax.axis_index("tbl").astype(jnp.int32).reshape(1)
    grp = lax.axis_index("grp").astype(jnp.int32).reshape(1)
    counts, target, place = pl.pallas_call(
        functools.partial(count_kernel, order),
        out_shape=[
            jax.ShapeDtypeStruct((samples, held), F32),
            jax.ShapeDtypeStruct((samples, held), F32),
            jax.ShapeDtypeStruct((tbl_count, tbl_count), F32),
        ],
        in_specs=[SMEM, SMEM, VMEM, VMEM, VMEM, VMEM],
        out_specs=[VMEM, VMEM, VMEM],
        scratch_shapes=[
            pltpu.VMEM((samples, history), jnp.int32),
            pltpu.VMEM((samples, LANES), jnp.int32),
        ],
        cost_estimate=pl.CostEstimate(flops=100_000_000, bytes_accessed=1_000_000, transcendentals=0),
        compiler_params=SMALL,
        name="count",
    )(
        tbl,
        grp,
        history_ids[:, 0, :].T,
        history_lengths.T,
        query_items.T,
        slot_tables.reshape(1, tbl_count),
    )
    masked = pl.pallas_call(
        query_kernel,
        out_shape=jax.ShapeDtypeStruct((side, samples + SCALE_ROWS, width), BF16),
        in_specs=[VMEM, VMEM],
        out_specs=VMEM,
        compiler_params=SMALL,
        name="query",
    )(table, target)
    query = exchange(masked, across_rows)
    partial = pl.pallas_call(
        pool_kernel,
        out_shape=jax.ShapeDtypeStruct((side, 2 * (samples // side), width), BF16),
        in_specs=[VMEM, VMEM, VMEM],
        out_specs=VMEM,
        scratch_shapes=[pltpu.VMEM((samples, held), F32)],
        compiler_params=SMALL,
        name="pool",
    )(table, counts, query)
    got = exchange(partial, across_rows)
    pooled = pl.pallas_call(
        merge_kernel,
        out_shape=jax.ShapeDtypeStruct((tbl_count, width // LANES, LANES), BF16),
        in_specs=[VMEM],
        out_specs=VMEM,
        compiler_params=SMALL,
        name="merge",
    )(got)
    arrived = exchange(pooled, along_tbl)
    return pl.pallas_call(
        functools.partial(order_kernel, tbl_order),
        out_shape=jax.ShapeDtypeStruct((1, tbl_count, width), BF16),
        in_specs=[VMEM, VMEM],
        out_specs=VMEM,
        compiler_params=SMALL,
        name="order",
    )(place, arrived)


def solution(mesh):
    placed = (
        P("tbl", "grp", None),
        P("tbl", "grp"),
        P(None, "tbl"),
        P(None, "tbl", None),
        P(None, "tbl"),
        P(),
    )
    return jax.shard_map(
        per_device,
        mesh=mesh,
        in_specs=placed,
        out_specs=P(("tbl", "grp"), None, None),
        check_vma=False,
    )
```

```python
import functools

import jax
import jax.numpy as jnp
from jax import lax
from jax.experimental import pallas as pl
from jax.experimental.pallas import tpu as pltpu
from jax.sharding import PartitionSpec as P

F32 = jnp.float32
BF16 = jnp.bfloat16
VMEM = pl.BlockSpec(memory_space=pltpu.VMEM)
SMEM = pl.BlockSpec(memory_space=pltpu.SMEM)
HBM = pl.BlockSpec(memory_space=pltpu.HBM)
SMALL = pltpu.CompilerParams(vmem_limit_bytes=16 << 20)
SCALE_ROWS = 8
LANES = 128
CHIPS_SIDE = 4


def rotated(count, first):
    return [(place + first) % count for place in range(count)]


def pack_kernel(codes_ref, scales_ref, out_ref, block_ref, scale_ref, sems):
    copies = out_ref.shape[0]
    rows, width = codes_ref.shape
    fetch = [
        pltpu.make_async_copy(codes_ref, block_ref.at[pl.ds(0, rows)], sems.at[copies]),
        pltpu.make_async_copy(scales_ref, scale_ref, sems.at[copies + 1]),
    ]
    for move in fetch:
        move.start()
    fetch[1].wait()
    scale = scale_ref[...]
    high = scale.astype(BF16)
    rest = scale - high.astype(F32)
    middle = rest.astype(BF16)
    low = (rest - middle.astype(F32)).astype(BF16)
    place = lax.broadcasted_iota(jnp.int32, (SCALE_ROWS, width), 0)
    terms = jnp.where(
        place == 0,
        high.astype(F32),
        jnp.where(place == 1, middle.astype(F32), jnp.where(place == 2, low.astype(F32), 0.0)),
    ).astype(BF16)
    block_ref[rows:, :] = terms
    fetch[0].wait()
    moves = [
        pltpu.make_async_copy(block_ref, out_ref.at[copy], sems.at[copy]) for copy in range(copies)
    ]
    for move in moves:
        move.start()
    for move in moves:
        move.wait()


def count_kernel(
    order,
    tbl_ref,
    grp_ref,
    ids_ref,
    lengths_ref,
    items_ref,
    tables_ref,
    counts_ref,
    target_ref,
    place_ref,
    names_ref,
    item_ref,
):
    tbl_order, side_order = order
    history, batch = ids_ref.shape
    samples, held = counts_ref.shape
    tbl_count, side = len(tbl_order), len(side_order)
    rows = held // side
    turned = tbl_ref[0] % 2 == 0

    def split(grp):
        y, x = grp // side, grp % side
        return jnp.where(turned, y, x), jnp.where(turned, x, y)

    along, across = split(grp_ref[0])
    ids = ids_ref[...]
    items = items_ref[...]
    extra = jnp.concatenate(
        [
            lengths_ref[...],
            lax.shift_right_logical(items, 6),
            jnp.bitwise_and(items, 63),
            jnp.zeros((5, batch), jnp.int32),
        ],
        axis=0,
    )
    digits = jnp.concatenate(
        [lax.shift_right_logical(ids, 6), jnp.bitwise_and(ids, 63), extra], axis=0
    )
    digits = digits.astype(F32).astype(BF16)
    sample = lax.broadcasted_iota(jnp.int32, (samples, batch), 0)
    column = lax.broadcasted_iota(jnp.int32, (samples, batch), 1)
    tbl_at = (sample % tbl_count + tbl_order[0]) % tbl_count
    across_at = (sample // tbl_count + side_order[0]) % side
    grp_at = jnp.where(turned, along * side + across_at, across_at * side + along)
    chosen = jnp.where(column == tbl_at * side * side + grp_at, 1.0, 0.0).astype(BF16)
    own = lax.dot_general(chosen, digits, (((1,), (1,)), ((), ())), preferred_element_type=F32)

    def held_at(high, low):
        row = (high * 64.0 + low).astype(jnp.int32)
        owner_along, owner_across = split(row // rows)
        block = (owner_along - side_order[0] + side) % side
        return jnp.where(owner_across == across, block * rows + row % rows, -1)

    own_lengths = own[:, 2 * history : 2 * history + 1].astype(jnp.int32)
    position = lax.broadcasted_iota(jnp.int32, (samples, history), 1)
    names = held_at(own[:, :history], own[:, history : 2 * history])
    names_ref[...] = jnp.where(position < own_lengths, names, -1)
    item = held_at(
        own[:, 2 * history + 1 : 2 * history + 2], own[:, 2 * history + 2 : 2 * history + 3]
    )
    item_ref[...] = jnp.broadcast_to(item, item_ref.shape)
    lane = lax.broadcasted_iota(jnp.int32, (16, LANES), 1)
    one = jnp.ones((16, LANES), BF16)
    none = jnp.zeros((16, LANES), BF16)

    def group(k, carry):
        at = pl.ds(pl.multiple_of(k * 16, 16), 16)
        named = names_ref[at, :]
        named = [
            jnp.broadcast_to(named[:, h : h + 1], (16, LANES)).astype(jnp.int16)
            for h in range(history)
        ]
        item = item_ref[at, :]
        for first in range(0, held, LANES):
            row = (lane + first).astype(jnp.int16)
            total = none
            for h in range(history):
                total = total + jnp.where(named[h] == row, one, none)
            counts_ref[at, first : first + LANES] = total.astype(F32)
            target_ref[at, first : first + LANES] = jnp.where(item == lane + first, 1.0, 0.0)
        return carry

    lax.fori_loop(0, samples // 16, group, 0)
    table = lax.broadcasted_iota(jnp.int32, place_ref.shape, 0)
    place_ref[...] = jnp.where(table == tables_ref[...], 1.0, 0.0)


def query_kernel(table_ref, target_ref, out_ref):
    copies, height, width = out_ref.shape
    blocks = table_ref.shape[0]
    rows = table_ref.shape[1] - SCALE_ROWS
    samples = target_ref.shape[0]
    codes = jnp.zeros((samples, width), F32)
    terms = jnp.zeros((SCALE_ROWS, samples), F32)
    for block in range(blocks):
        target = target_ref[:, block * rows : (block + 1) * rows].astype(BF16)
        codes = codes + jnp.dot(target, table_ref[block, :rows, :], preferred_element_type=F32)
        terms = terms + lax.dot_general(
            table_ref[block, rows:, :],
            target,
            (((1,), (1,)), ((), ())),
            preferred_element_type=F32,
        )
    codes = codes.astype(BF16)
    terms = jnp.concatenate([terms, jnp.zeros((SCALE_ROWS, width - samples), F32)], axis=1)
    terms = terms.astype(BF16)
    for copy in range(copies):
        out_ref[copy, :samples, :] = codes
        out_ref[copy, samples:, :] = terms


def pool_kernel(table_ref, counts_ref, query_ref, out_ref, score_ref):
    blocks, height, width = table_ref.shape
    rows = height - SCALE_ROWS
    samples = counts_ref.shape[0]

    def scales(block):
        terms = table_ref[block, rows:, :].astype(F32)
        return terms[0:1] + (terms[1:2] + terms[2:3])

    def columns(block):
        return slice(block * rows, (block + 1) * rows)

    query = query_ref[0].astype(F32)
    for copy in range(1, query_ref.shape[0]):
        query = query + query_ref[copy].astype(F32)
    factor = query[samples:, :samples]
    factor = (factor[0:1] + (factor[1:2] + factor[2:3])) * (1.0 / width)
    factor = jnp.broadcast_to(factor, (samples, samples)).T
    factor = jnp.concatenate([factor] * (rows // samples), axis=1)
    query = query[:samples].astype(BF16)
    top = jnp.full((samples, rows), -1e30, F32)
    for block in range(blocks):
        raw = lax.dot_general(
            query, table_ref[block, :rows, :], (((1,), (1,)), ((), ())), preferred_element_type=F32
        )
        score = raw * scales(block) * factor
        score = jnp.where(counts_ref[:, columns(block)] > 0.0, score, -1e30)
        score_ref[:, columns(block)] = score
        top = jnp.maximum(top, score)
    peak = jnp.max(top, axis=1, keepdims=True)
    mass = jnp.zeros((samples, rows), F32)
    pooled = jnp.zeros((2 * samples, width), F32)
    for block in range(blocks):
        weight = counts_ref[:, columns(block)] * jnp.exp(score_ref[:, columns(block)] - peak)
        mass = mass + weight
        scaled = weight * scales(block)
        high = scaled.astype(BF16)
        low = (scaled - high.astype(F32)).astype(BF16)
        pooled = pooled + jnp.dot(
            jnp.concatenate([high, low], axis=0),
            table_ref[block, :rows, :],
            preferred_element_type=F32,
        )
    mass = jnp.sum(mass, axis=1, keepdims=True)
    pooled = pooled[:samples] + pooled[samples:]
    lane = lax.broadcasted_iota(jnp.int32, (samples, LANES), 1)
    last = jnp.where(lane == 0, peak, mass)
    size = out_ref.shape[1]
    for block in range(out_ref.shape[0]):
        out_ref[block, :, :width] = pooled[block * size : (block + 1) * size]
        out_ref[block, :, width:] = last[block * size : (block + 1) * size]


def merge_kernel(got_ref, out_ref):
    count = got_ref.shape[0]
    width = got_ref.shape[2] - LANES
    peaks = [got_ref[k, :, width : width + 1] for k in range(count)]
    top = functools.reduce(jnp.maximum, peaks)
    shift = [jnp.exp(peak - top) for peak in peaks]
    mass = sum(f * got_ref[k, :, width + 1 : width + 2] for k, f in enumerate(shift))
    pooled = sum(f * got_ref[k, :, :width] for k, f in enumerate(shift)) / mass
    pooled = pooled.astype(BF16)
    for part in range(width // LANES):
        out_ref[:, part, :] = pooled[:, part * LANES : (part + 1) * LANES]


def order_kernel(tbl_order, place_ref, pooled_ref, out_ref):
    slots, parts, lanes = pooled_ref.shape
    first = slots - tbl_order[0]
    place = place_ref[...].astype(BF16)
    for part in range(parts):
        rows = pooled_ref[:, part, :]
        rows = jnp.concatenate([rows[first:], rows[:first]], axis=0)
        ordered = jnp.dot(place, rows, preferred_element_type=F32).astype(BF16)
        out_ref[0, :, part * lanes : (part + 1) * lanes] = ordered


def per_device(codes, row_scales, history_lengths, history_ids, query_items, slot_tables):
    _, rows, width = codes.shape
    batch, _, history = history_ids.shape
    tbl_count = lax.axis_size("tbl")
    grp_count = lax.axis_size("grp")
    side = CHIPS_SIDE
    samples = tbl_count * side
    held = rows * side
    tbl_order = rotated(tbl_count, tbl_count // 2 + 5)
    side_order = rotated(side, side // 2)
    order = (tbl_order, side_order)
    tables, places = range(tbl_count), range(side)

    def device(t, along, across):
        y, x = (across, along) if t % 2 else (along, across)
        return (t * side + y) * side + x

    along_rows = [[device(t, u, v) for u in side_order] for t in tables for v in places]
    across_rows = [[device(t, u, v) for v in side_order] for t in tables for u in places]
    along_tbl = [[t * grp_count + g for t in tbl_order] for g in range(grp_count)]

    def exchange(blocks, groups):
        return lax.all_to_all(
            blocks, ("tbl", "grp"), 0, 0, axis_index_groups=groups, tiled=True
        )

    packed = pl.pallas_call(
        pack_kernel,
        out_shape=jax.ShapeDtypeStruct((side, rows + SCALE_ROWS, width), BF16),
        in_specs=[HBM, HBM],
        out_specs=HBM,
        scratch_shapes=[
            pltpu.VMEM((rows + SCALE_ROWS, width), BF16),
            pltpu.VMEM((1, rows), F32),
            pltpu.SemaphoreType.DMA((side + 2,)),
        ],
        name="pack",
    )(codes[0], row_scales)
    table = exchange(packed, along_rows)
    tbl = lax.axis_index("tbl").astype(jnp.int32).reshape(1)
    grp = lax.axis_index("grp").astype(jnp.int32).reshape(1)
    counts, target, place = pl.pallas_call(
        functools.partial(count_kernel, order),
        out_shape=[
            jax.ShapeDtypeStruct((samples, held), F32),
            jax.ShapeDtypeStruct((samples, held), F32),
            jax.ShapeDtypeStruct((tbl_count, tbl_count), F32),
        ],
        in_specs=[SMEM, SMEM, VMEM, VMEM, VMEM, VMEM],
        out_specs=[VMEM, VMEM, VMEM],
        scratch_shapes=[
            pltpu.VMEM((samples, history), jnp.int32),
            pltpu.VMEM((samples, LANES), jnp.int32),
        ],
        cost_estimate=pl.CostEstimate(flops=100_000_000, bytes_accessed=1_000_000, transcendentals=0),
        compiler_params=SMALL,
        name="count",
    )(
        tbl,
        grp,
        history_ids[:, 0, :].T,
        history_lengths.T,
        query_items.T,
        slot_tables.reshape(1, tbl_count),
    )
    masked = pl.pallas_call(
        query_kernel,
        out_shape=jax.ShapeDtypeStruct((side, samples + SCALE_ROWS, width), BF16),
        in_specs=[VMEM, VMEM],
        out_specs=VMEM,
        compiler_params=SMALL,
        name="query",
    )(table, target)
    query = exchange(masked, across_rows)
    partial = pl.pallas_call(
        pool_kernel,
        out_shape=jax.ShapeDtypeStruct((side, samples // side, width + LANES), F32),
        in_specs=[VMEM, VMEM, VMEM],
        out_specs=VMEM,
        scratch_shapes=[pltpu.VMEM((samples, held), F32)],
        compiler_params=SMALL,
        name="pool",
    )(table, counts, query)
    got = exchange(partial, across_rows)
    pooled = pl.pallas_call(
        merge_kernel,
        out_shape=jax.ShapeDtypeStruct((tbl_count, width // LANES, LANES), BF16),
        in_specs=[VMEM],
        out_specs=VMEM,
        compiler_params=SMALL,
        name="merge",
    )(got)
    arrived = exchange(pooled, along_tbl)
    return pl.pallas_call(
        functools.partial(order_kernel, tbl_order),
        out_shape=jax.ShapeDtypeStruct((1, tbl_count, width), BF16),
        in_specs=[VMEM, VMEM],
        out_specs=VMEM,
        compiler_params=SMALL,
        name="order",
    )(place, arrived)


def solution(mesh):
    placed = (
        P("tbl", "grp", None),
        P("tbl", "grp"),
        P(None, "tbl"),
        P(None, "tbl", None),
        P(None, "tbl"),
        P(),
    )
    return jax.shard_map(
        per_device,
        mesh=mesh,
        in_specs=placed,
        out_specs=P(("tbl", "grp"), None, None),
        check_vma=False,
    )
```
